32 devices in a mesh: group: 2 (over core), blk: 16 (over z, y, x).
Axes of the slice: x: 2, y: 2, z: 4, core: 2. Of those that a mesh axis runs over, the one named last changes fastest.
Arguments:
- field: float32 [2, 16, 5, 32, 512], P('group', 'blk'), may hold values from -6 to 6
- source: float32 [2, 16, 5, 32, 512], P('group', 'blk'), may hold values from -6 to 6
- block_inverse: float32 [2, 16, 5, 5, 32, 512], P('group', 'blk'), may hold values from -0.05 to 0.14, as said below
- coupling: float32 [2, 16, 4, 32, 512], P('group', 'blk'), may hold values from 0.3 to 1.2
- donor_base: int32 [2, 16, 16, 256], P('group', 'blk'), may hold values from 0 to 15870
- donor_weight: float32 [2, 16, 4, 16, 256], P('group', 'blk'), may hold values from 0 to 1, as said below
- receiver_cell: int32 [2, 16, 16, 256], P('group', 'blk'), may hold values from 0 to 16384, as said below
Outputs:
- field_out: float32 [2, 16, 5, 32, 512], P('group', 'blk')
The draws below stay inside these ranges and needn't reach their ends.
Inputs may be any that keep to these rules, and one draw needn't show every extreme that they name: `block_inverse`: the entries of a block diagonal lie in 0.06 to 0.14; other entries are at most 0.05 in magnitude. `donor_weight`: the four weights of a slot are positive and sum to one. `receiver_cell`: within one block all entries below 16384 are distinct cells; for each donor block the used slots come first and the rest hold 16384; in every block some donor block fills all 256 slots.
All inputs are finite; a program needn't handle non-finite values.
Results may differ from the reference program's by a relative error of at most 0.0003.
Values sent between devices are 32-bit elements; how exact they have to be, the bound alone decides.
No kernel may reach another device: no remote copies, remote signals or barrier semaphores. Data moves between devices by JAX's collectives and lax.ppermute only.
A program may use at most 128 MiB of HBM per device.

```python
import math
from functools import partial
import jax
import jax.numpy as jnp

NJ = 32
NK = 512
COMPONENTS = 5
SLOTS = 256
ITERS = 4
BLOCKS = 16
N_GROUP = 2


def draw_block_inverse(key, part):
    first, second = jax.random.split(jax.random.fold_in(key, 11))
    shape = (2, BLOCKS, COMPONENTS, COMPONENTS, NJ, NK)
    diag_shape = (2, BLOCKS, COMPONENTS, NJ, NK)
    diagonal = jnp.exp(jax.random.uniform(first, diag_shape, jnp.float32, math.log(0.06), math.log(0.14)))
    others = jnp.clip(0.015 * jax.random.normal(second, shape, jnp.float32), -0.05, 0.05)
    identity = jnp.eye(COMPONENTS, dtype=jnp.float32)[:, :, None, None]
    return others * (1.0 - identity) + identity * diagonal[:, :, :, None]


def draw_donor_weight(key, part):
    lower = 0.1
    raw = jax.random.uniform(jax.random.fold_in(key, 23), (2, BLOCKS, 4, BLOCKS, SLOTS), jnp.float32, lower, 1.0)
    return raw / jnp.sum(raw, axis=2, keepdims=True)


def receivers_of_block(key):
    first, second, third = jax.random.split(key, 3)
    cell_count = NJ * NK
    chosen = jax.random.permutation(first, cell_count)[:BLOCKS * SLOTS].reshape(BLOCKS, SLOTS).astype(jnp.int32)
    drawn = jax.random.randint(second, (BLOCKS,), 0, SLOTS + 1)
    counts = drawn * drawn // SLOTS
    fullest = jax.random.randint(third, (), 0, BLOCKS)
    counts = jnp.where(jnp.arange(BLOCKS) == fullest, SLOTS, counts)
    slot_iota = jnp.arange(SLOTS)
    return jnp.where(slot_iota[None, :] < counts[:, None], chosen, cell_count).astype(jnp.int32)


def draw_receiver_cell(key, part):
    keys = jax.random.split(jax.random.fold_in(key, 37), 2 * BLOCKS)
    return jax.vmap(receivers_of_block)(keys).reshape(2, BLOCKS, BLOCKS, SLOTS)


def set_ends(entries, rng, smallest, high):
    spot = [jax.random.randint(jax.random.fold_in(rng, axis), (), 0, length) for axis, length in enumerate(entries.shape)]
    main_axis = entries.shape.index(max(entries.shape))
    neighbour = spot[:main_axis] + [(spot[main_axis] + 1) % entries.shape[main_axis]] + spot[main_axis + 1:]
    return entries.at[tuple(spot)].set(smallest).at[tuple(neighbour)].set(high)


def shard_levels(key, extent, cuts, least, top_value):
    gain, own = 1.0, jax.random.fold_in(key, 6)
    for dim, parts in cuts:
        steps = jnp.exp(jax.random.uniform(jax.random.fold_in(own, dim), (parts,), jnp.float32, least / len(cuts), top_value / len(cuts)))
        gain = gain * jnp.repeat(steps, extent[dim] // parts).reshape([-1 if axis == dim else 1 for axis in range(len(extent))])
    return gain


def centred(stream_key, dims, scale, most, cuts=(), held_as=jnp.bfloat16):
    factor_of = shard_levels(stream_key, dims, cuts, -0.22, 0.18) if cuts else 1.0
    entries = jax.random.normal(stream_key, dims, jnp.float32) * scale * factor_of
    return jnp.minimum(jnp.maximum(entries, -most), most).astype(held_as)


def setup_inputs(seed: int = 0) -> dict:
    splits = jax.random.split(jax.random.key(seed), 8)
    field = centred(splits[0], (N_GROUP, BLOCKS, COMPONENTS, NJ, NK), 1.0, 6.0, ((0, 2), (1, 16)), jnp.float32)
    source = centred(splits[1], (N_GROUP, BLOCKS, COMPONENTS, NJ, NK), 1.0, 6.0, ((0, 2), (1, 16)), jnp.float32)
    block_inverse = draw_block_inverse(jax.random.fold_in(splits[7], 71), 0)
    coupling = jnp.clip(jnp.exp(math.log(1.2) - 1.3862944 * jax.random.uniform(splits[3], (N_GROUP, BLOCKS, 4, NJ, NK), jnp.float32) ** shard_levels(splits[3], (N_GROUP, BLOCKS, 4, NJ, NK), ((0, 2), (1, 16)), -0.2, 0.2)), 0.3, 1.2)
    donor_base = set_ends(jax.random.randint(splits[4], (N_GROUP, BLOCKS, BLOCKS, SLOTS), 0, (NJ - 1) * NK - 1), jax.random.fold_in(splits[4], 1), 0, ((NJ - 1) * NK - 1) - 1).astype(jnp.int32)
    donor_weight = draw_donor_weight(jax.random.fold_in(splits[7], 71), 0)
    receiver_cell = draw_receiver_cell(jax.random.fold_in(splits[7], 71), 0)
    return {"field": field, "source": source, "block_inverse": block_inverse, "coupling": coupling, "donor_base": donor_base, "donor_weight": donor_weight, "receiver_cell": receiver_cell}


upwind_offsets = (-3, -2, -1, 0, 1, 2)
upwind_weights = (-2.0 / 60.0, 15.0 / 60.0, -60.0 / 60.0, 20.0 / 60.0, 30.0 / 60.0, -3.0 / 60.0)


def window(padded, shift_j, shift_k, row_count, column_count):
    return padded[:, 3 + shift_j:3 + shift_j + row_count, 3 + shift_k:3 + shift_k + column_count]


def near_half(padded, solution, forcing, inverse, coupling, update_mask):
    row_count, column_count = solution.shape[1], solution.shape[2]
    gathered = coupling[0] * window(padded, -1, 0, row_count, column_count)
    gathered = gathered + coupling[1] * window(padded, 1, 0, row_count, column_count)
    gathered = gathered + coupling[2] * window(padded, 0, -1, row_count, column_count)
    gathered = gathered + coupling[3] * window(padded, 0, 1, row_count, column_count)
    total = forcing + gathered
    updated = jnp.sum(inverse * total[None], axis=1)
    return jnp.where(update_mask[None], updated, solution)


def off_section(padded, solution, forcing, inverse, coupling, update_mask):
    row_count, column_count = solution.shape[1], solution.shape[2]
    along_j = jnp.zeros_like(solution)
    along_k = jnp.zeros_like(solution)
    for offset, weight in zip(upwind_offsets, upwind_weights):
        along_j = along_j + weight * window(padded, offset, 0, row_count, column_count)
        along_k = along_k + weight * window(padded, 0, offset, row_count, column_count)
    residual_term = forcing - coupling[0] * along_j - coupling[1] * along_k
    updated = solution + jnp.sum(inverse * residual_term[None], axis=1)
    return jnp.where(update_mask[None], updated, solution)


def interpolate(flat_state, bases, weights, column_count):
    result = jnp.zeros((flat_state.shape[0],) + bases.shape, jnp.float32)
    for corner, offset in enumerate((0, 1, column_count, column_count + 1)):
        result = result + weights[corner][None] * flat_state[:, bases + offset]
    return result


def place(flat_state, targets, values):
    return flat_state.at[:, targets].set(values, mode="drop")


def mark(targets, cell_count):
    return jnp.zeros(cell_count, jnp.int32).at[targets].set(1, mode="drop")


def to_grid(array):
    moved = jnp.moveaxis(array, 0, -3)
    return moved.reshape(moved.shape[:-3] + (moved.shape[-3] * moved.shape[-2], moved.shape[-1]))


def from_grid(grid, block_count):
    pieces = grid.reshape(grid.shape[:-2] + (block_count, grid.shape[-2] // block_count, grid.shape[-1]))
    return jnp.moveaxis(pieces, -3, 0)


def pad_grid(grid):
    return jnp.pad(grid, ((0, 0), (3, 3), (3, 3)))


def reference(field, source, block_inverse, coupling, donor_base, donor_weight, receiver_cell):
    cell_count = NJ * NK
    targets = receiver_cell.reshape(2, BLOCKS, BLOCKS * SLOTS)
    frozen = jax.vmap(jax.vmap(partial(mark, cell_count=cell_count)))(targets).reshape(2, BLOCKS, NJ, NK)
    movable = [to_grid(frozen[0]) == 0, to_grid(frozen[1]) == 0]
    rows_iota = jax.lax.broadcasted_iota(jnp.int32, (BLOCKS * NJ, NK), 0)
    cols_iota = jax.lax.broadcasted_iota(jnp.int32, (BLOCKS * NJ, NK), 1)
    parity_grid = (rows_iota + cols_iota) % 2
    forcing = [to_grid(source[0]), to_grid(source[1])]
    inverse = [to_grid(block_inverse[0]), to_grid(block_inverse[1])]
    factors = [to_grid(coupling[0]), to_grid(coupling[1])]
    solution = field
    for iteration in range(ITERS):
        flat_state = solution.reshape(2, BLOCKS, COMPONENTS, cell_count)
        donor_values = jax.vmap(jax.vmap(partial(interpolate, column_count=NK)))(flat_state, donor_base, donor_weight)
        arrived = jnp.transpose(donor_values[::-1], (0, 3, 2, 1, 4)).reshape(2, BLOCKS, COMPONENTS, BLOCKS * SLOTS)
        flat_state = jax.vmap(jax.vmap(place))(flat_state, targets, arrived)
        solution = flat_state.reshape(2, BLOCKS, COMPONENTS, NJ, NK)
        near_grid = to_grid(solution[0])
        off_grid = to_grid(solution[1])
        for parity in range(2):
            near_grid = near_half(pad_grid(near_grid), near_grid, forcing[0], inverse[0], factors[0], movable[0] & (parity_grid == parity))
            off_grid = off_section(pad_grid(off_grid), off_grid, forcing[1], inverse[1], factors[1], movable[1])
        solution = jnp.stack([from_grid(near_grid, BLOCKS), from_grid(off_grid, BLOCKS)])
    return solution
```

```python
from functools import partial

import jax
import jax.numpy as jnp
from jax import lax
from jax.experimental import pallas as pl
from jax.experimental.pallas import tpu as pltpu
from jax.sharding import PartitionSpec as P

ITERS = 4

upwind_offsets = (-3, -2, -1, 0, 1, 2)
upwind_weights = (-2.0 / 60.0, 15.0 / 60.0, -60.0 / 60.0, 20.0 / 60.0, 30.0 / 60.0, -3.0 / 60.0)

F32 = jnp.float32
BF16 = jnp.bfloat16
ROWS = 8
LOW, HIGH = 6, 4
LOW_DONE, HIGH_DONE = 3, 2
PAD = 2 * ROWS


def vmem(count):
    return [pl.BlockSpec(memory_space=pltpu.VMEM)] * count


def divmod_const(value, size):
    if size & (size - 1) == 0:
        return value >> (size.bit_length() - 1), value & (size - 1)
    quotient = lax.div(value, jnp.int32(size))
    return quotient, value - quotient * size


def one_hot(index, size):
    rows = lax.broadcasted_iota(jnp.int32, (size, index.shape[1]), 0)
    return jnp.where(rows == index, 1.0, 0.0).astype(BF16)


def split(value):
    high = value.astype(BF16)
    low = (value - high.astype(F32)).astype(BF16)
    return high, low


def donor_sums(state, base_ref, weight_ref, out_ref):
    comps, rows, cols = state.shape
    half = cols // 2
    flat = state.reshape(comps * rows, cols)
    stacked = jnp.concatenate(split(flat), axis=0)
    at = lax.broadcasted_iota(jnp.int32, (cols, cols), 0)
    to = lax.broadcasted_iota(jnp.int32, (cols, cols), 1)
    source_col = jnp.where(to < half, 2 * to, 2 * (to - half) + 1)
    order = jnp.where(at == source_col, 1.0, 0.0).astype(BF16)
    ordered = jnp.dot(stacked, order, preferred_element_type=F32).astype(BF16)
    even, odd = ordered[:, :half], ordered[:, half:]
    slots = base_ref.shape[1]
    row_iota = lax.broadcasted_iota(jnp.int32, (rows, slots), 0)

    def one(d, carry):
        base = base_ref[pl.ds(d, 1), :]
        w0 = weight_ref[0, pl.ds(d, 1), :]
        w1 = weight_ref[1, pl.ds(d, 1), :]
        w2 = weight_ref[2, pl.ds(d, 1), :]
        w3 = weight_ref[3, pl.ds(d, 1), :]
        row, col = divmod_const(base, cols)
        is_odd = (col & 1) == 1
        wraps = col == cols - 1
        odd_at = col >> 1
        even_at = jnp.where(wraps, 0, (col + 1) >> 1)
        even_row = row + jnp.where(wraps, 1, 0)
        picked_even = jnp.dot(even, one_hot(even_at, half), preferred_element_type=F32)
        picked_odd = jnp.dot(odd, one_hot(odd_at, half), preferred_element_type=F32)
        count = comps * rows
        picked_even = (picked_even[:count] + picked_even[count:]).reshape(comps, rows, slots)
        picked_odd = (picked_odd[:count] + picked_odd[count:]).reshape(comps, rows, slots)
        even_weight = jnp.where(
            row_iota == even_row,
            jnp.where(is_odd, w1, w0),
            jnp.where(row_iota == even_row + 1, jnp.where(is_odd, w3, w2), 0.0),
        )
        odd_weight = jnp.where(
            row_iota == row,
            jnp.where(is_odd, w0, w1),
            jnp.where(row_iota == row + 1, jnp.where(is_odd, w2, w3), 0.0),
        )
        total = even_weight[None] * picked_even + odd_weight[None] * picked_odd
        out_ref[d, 0:comps, :] = jnp.sum(total, axis=1)
        return carry

    lax.fori_loop(0, base_ref.shape[0], one, 0)


def spread(values_of, target_ref, comps, rows, cols, acc_ref, exact):
    slots = target_ref.shape[1]
    row_iota = lax.broadcasted_iota(jnp.int32, (rows, slots), 0)
    acc_ref[...] = jnp.zeros_like(acc_ref)

    def one(b, carry):
        row, col = divmod_const(target_ref[pl.ds(b, 1), :], cols)
        hit = row_iota == row
        columns = one_hot(col, cols)
        values = values_of(b)
        parts = [values] if exact else [values.astype(BF16).astype(F32)]
        if not exact:
            parts.append(values - parts[0])
        placed = [
            jnp.where(hit[None], part[:, None, :], 0.0).reshape(comps * rows, slots).astype(BF16)
            for part in parts
        ]
        left = jnp.concatenate(placed, axis=1)
        right = jnp.concatenate([columns] * len(parts), axis=1)
        acc_ref[...] += lax.dot_general(
            left, right, (((1,), (1,)), ((), ())), preferred_element_type=F32
        )
        return carry

    lax.fori_loop(0, target_ref.shape[0], one, 0)


def start_kernel(field_ref, base_ref, weight_ref, target_ref, out_ref, movable_ref, acc_ref):
    rows, cols = field_ref.shape[1:]
    donor_sums(field_ref[...], base_ref, weight_ref, out_ref)
    slots = target_ref.shape[1]
    spread(lambda b: jnp.ones((1, slots), F32), target_ref, 1, rows, cols, acc_ref, True)
    movable_ref[...] = jnp.where(acc_ref[...] > 0.5, 0.0, 1.0)


def place_kernel(arrived_ref, target_ref, state_ref, movable_ref, out_ref, top_ref, bottom_ref, acc_ref):
    comps, rows, cols = state_ref.shape
    spread(
        lambda b: arrived_ref[b, 0:comps, :], target_ref, comps, rows, cols, acc_ref, False
    )
    movable = movable_ref[...] > 0.5
    for c in range(comps):
        placed = acc_ref[c * rows : (c + 1) * rows, :]
        new = jnp.where(movable, state_ref[c], placed)
        out_ref[c] = new
        top_ref[c * LOW : (c + 1) * LOW, :] = new[rows - LOW :, :]
        bottom_ref[c * HIGH : (c + 1) * HIGH, :] = new[:HIGH, :]


def sections(u_ref, start, parts, write, is_near, parity, comps, cols):
    source, inverse, coupling, movable = parts
    lanes = lax.broadcasted_iota(jnp.int32, (ROWS, cols), 1)
    sublanes = lax.broadcasted_iota(jnp.int32, (ROWS, cols), 0)

    def rows_at(c, offset):
        return u_ref[c, start + offset : start + offset + ROWS, :]

    def shifted(value, offset):
        return pltpu.roll(value, (-offset) % cols, 1)

    def finish(update, terms, mask):
        for v in range(comps):
            total = update(v)
            for w in range(comps):
                product = inverse(v, w) * terms[w]
                total = product if total is None else total + product
            write(v, jnp.where(mask, total, rows_at(v, 0)))

    @pl.when(is_near)
    def _():
        c0, c1, c2, c3 = (coupling(i) for i in range(4))
        c2 = jnp.where(lanes >= 1, c2, 0.0)
        c3 = jnp.where(lanes < cols - 1, c3, 0.0)
        terms = []
        for w in range(comps):
            here = rows_at(w, 0)
            term = source(w) + c0 * rows_at(w, -1) + c1 * rows_at(w, 1)
            terms.append(term + c2 * shifted(here, -1) + c3 * shifted(here, 1))
        colour = ((lanes + sublanes) & 1) == parity
        finish(lambda v: None, terms, colour & (movable() > 0.5))

    @pl.when(jnp.logical_not(is_near))
    def _():
        c0, c1 = coupling(0), coupling(1)
        factors = []
        for offset, weight in zip(upwind_offsets, upwind_weights):
            inside = (lanes + offset >= 0) & (lanes + offset < cols)
            factors.append(weight if offset == 0 else jnp.where(inside, weight, 0.0))
        terms = []
        for w in range(comps):
            here = rows_at(w, 0)
            along_j = along_k = None
            for offset, weight, factor in zip(upwind_offsets, upwind_weights, factors):
                in_j = weight * rows_at(w, offset)
                in_k = factor * (here if offset == 0 else shifted(here, offset))
                along_j = in_j if along_j is None else along_j + in_j
                along_k = in_k if along_k is None else along_k + in_k
            terms.append(source(w) - c0 * along_j - c1 * along_k)
        finish(lambda v: rows_at(v, 0), terms, movable() > 0.5)


def sweep(
    state_ref, below_ref, above_ref, source_ref, inverse_ref, coupling_ref, movable_ref,
    low_ref, high_ref, u_ref, v_ref, out_ref,
):
    comps, rows, cols = state_ref.shape
    is_near = lax.axis_index("group") == 0
    for c in range(comps):
        u_ref[c, PAD : PAD + rows, :] = state_ref[c]
        u_ref[c, PAD - LOW : PAD, :] = below_ref[c * LOW : (c + 1) * LOW, :]
        u_ref[c, PAD + rows : PAD + rows + HIGH, :] = above_ref[c * HIGH : (c + 1) * HIGH, :]
        v_ref[c, 0:PAD, :] = jnp.zeros((PAD, cols), F32)
        v_ref[c, PAD + rows :, :] = jnp.zeros((PAD, cols), F32)

    def own(r):
        at = slice(r, r + ROWS)
        return (
            lambda w: source_ref[w, at, :],
            lambda v, w: inverse_ref[v, w, at, :],
            lambda i: coupling_ref[i, at, :],
            lambda: movable_ref[at, :],
        )

    def packed(ref):
        first = comps * comps
        second = first + comps
        last = ref.shape[0] - 1
        return (
            lambda w: ref[first + w],
            lambda v, w: ref[v * comps + w],
            lambda i: ref[second + i],
            lambda: ref[last],
        )

    def into(ref, start):
        def write(v, value):
            ref[v, start : start + ROWS, :] = value
        return write

    sections(u_ref, PAD - ROWS, packed(low_ref), into(v_ref, PAD - ROWS), is_near, 0, comps, cols)
    for r in range(0, rows, ROWS):
        sections(u_ref, PAD + r, own(r), into(v_ref, PAD + r), is_near, 0, comps, cols)
    sections(u_ref, PAD + rows, packed(high_ref), into(v_ref, PAD + rows), is_near, 0, comps, cols)
    for r in range(0, rows, ROWS):
        sections(v_ref, PAD + r, own(r), into(out_ref, r), is_near, 1, comps, cols)


def middle_kernel(
    state_ref, below_ref, above_ref, source_ref, inverse_ref, coupling_ref, movable_ref,
    low_ref, high_ref, base_ref, weight_ref, out_ref, sums_ref, u_ref, v_ref,
):
    sweep(
        state_ref, below_ref, above_ref, source_ref, inverse_ref, coupling_ref, movable_ref,
        low_ref, high_ref, u_ref, v_ref, out_ref,
    )
    donor_sums(out_ref[...], base_ref, weight_ref, sums_ref)


def last_kernel(
    state_ref, below_ref, above_ref, source_ref, inverse_ref, coupling_ref, movable_ref,
    low_ref, high_ref, out_ref, u_ref, v_ref,
):
    sweep(
        state_ref, below_ref, above_ref, source_ref, inverse_ref, coupling_ref, movable_ref,
        low_ref, high_ref, u_ref, v_ref, out_ref,
    )


def on_device(field, source, block_inverse, coupling, donor_base, donor_weight, receiver_cell):
    state = field[0, 0]
    source = source[0, 0]
    inverse = block_inverse[0, 0]
    coupling = coupling[0, 0]
    base = donor_base[0, 0]
    weight = donor_weight[0, 0]
    target = receiver_cell[0, 0]
    comps, rows, cols = state.shape
    blocks, slots = base.shape
    groups = lax.axis_size("group")
    swap = [(g * blocks + b, (groups - 1 - g) * blocks + b) for g in range(groups) for b in range(blocks)]
    up = [(b, b + 1) for b in range(blocks - 1)]
    down = [(b + 1, b) for b in range(blocks - 1)]

    def f32(*shape):
        return jax.ShapeDtypeStruct(shape, F32)

    params = pltpu.CompilerParams(vmem_limit_bytes=48 * 1024 * 1024)
    sums_shape = f32(blocks, -(-comps // ROWS) * ROWS, slots)

    sums, movable = pl.pallas_call(
        start_kernel,
        out_shape=(sums_shape, f32(rows, cols)),
        in_specs=vmem(4),
        out_specs=tuple(vmem(2)),
        scratch_shapes=[pltpu.VMEM((rows, cols), F32)],
        compiler_params=params,
        name="start",
    )(state, base, weight, target)

    def fixed_rows(at, count):
        return jnp.concatenate(
            [
                inverse[:, :, at : at + count].reshape(comps * comps, count, cols),
                source[:, at : at + count],
                coupling[:, at : at + count],
                movable[None, at : at + count],
            ],
            axis=0,
        )

    low = lax.ppermute(fixed_rows(rows - LOW_DONE, LOW_DONE), "blk", up)
    high = lax.ppermute(fixed_rows(0, HIGH_DONE), "blk", down)
    low = jnp.pad(low, ((0, 0), (ROWS - LOW_DONE, 0), (0, 0)))
    high = jnp.pad(high, ((0, 0), (0, ROWS - HIGH_DONE), (0, 0)))

    working = [pltpu.VMEM((comps, rows + 2 * PAD, cols), F32)] * 2
    for iteration in range(ITERS):
        arrived = lax.ppermute(sums, ("group", "blk"), swap)
        arrived = lax.all_to_all(arrived, "blk", split_axis=0, concat_axis=0, tiled=True)
        state, top, bottom = pl.pallas_call(
            place_kernel,
            out_shape=(f32(comps, rows, cols), f32(comps * LOW, cols), f32(comps * HIGH, cols)),
            in_specs=vmem(4),
            out_specs=tuple(vmem(3)),
            scratch_shapes=[pltpu.VMEM((comps * rows, cols), F32)],
            compiler_params=params,
            name="place",
        )(arrived, target, state, movable)
        below = lax.ppermute(top, "blk", up)
        above = lax.ppermute(bottom, "blk", down)
        operands = (state, below, above, source, inverse, coupling, movable, low, high)
        if iteration < ITERS - 1:
            state, sums = pl.pallas_call(
                middle_kernel,
                out_shape=(f32(comps, rows, cols), sums_shape),
                in_specs=vmem(11),
                out_specs=tuple(vmem(2)),
                scratch_shapes=working,
                compiler_params=params,
                name="middle",
            )(*operands, base, weight)
        else:
            state = pl.pallas_call(
                last_kernel,
                out_shape=f32(comps, rows, cols),
                in_specs=vmem(9),
                out_specs=vmem(1)[0],
                scratch_shapes=working,
                compiler_params=params,
                name="last",
            )(*operands)
    return state[None, None]


def solution(mesh):
    in_specs = (
        P("group", "blk", None, None, None),
        P("group", "blk", None, None, None),
        P("group", "blk", None, None, None, None),
        P("group", "blk", None, None, None),
        P("group", "blk", None, None),
        P("group", "blk", None, None, None),
        P("group", "blk", None, None),
    )
    out_specs = P("group", "blk", None, None, None)
    return jax.shard_map(
        on_device, mesh=mesh, in_specs=in_specs, out_specs=out_specs, check_vma=False
    )
```

```python
from functools import partial

import jax
import jax.numpy as jnp
from jax import lax
from jax.experimental import pallas as pl
from jax.experimental.pallas import tpu as pltpu
from jax.sharding import PartitionSpec as P

ITERS = 4

upwind_offsets = (-3, -2, -1, 0, 1, 2)
upwind_weights = (-2.0 / 60.0, 15.0 / 60.0, -60.0 / 60.0, 20.0 / 60.0, 30.0 / 60.0, -3.0 / 60.0)

F32 = jnp.float32
BF16 = jnp.bfloat16
ROWS = 8
LOW, HIGH = 6, 4
LOW_DONE, HIGH_DONE = 3, 2
PAD = 2 * ROWS
LANES, LANE_BITS, GROUP_BITS = 128, 7, 2
UNROLL = 16
VMEM_LIMIT = 16 * 1024 * 1024


def vmem(count):
    return [pl.BlockSpec(memory_space=pltpu.VMEM)] * count


def divmod_const(value, size):
    if size & (size - 1) == 0:
        return value >> (size.bit_length() - 1), value & (size - 1)
    quotient = lax.div(value, jnp.int32(size))
    return quotient, value - quotient * size


def one_hot(index, size):
    rows = lax.broadcasted_iota(jnp.int32, (size, index.shape[1]), 0)
    return jnp.where(rows == index, 1.0, 0.0).astype(BF16)


def split(value):
    high = value.astype(BF16)
    low = (value - high.astype(F32)).astype(BF16)
    return high, low


def repeat(count, step, unroll=UNROLL):
    lax.fori_loop(0, count, lambda i, carry: (step(i), carry)[1], 0, unroll=min(count, unroll))


def donor_sums(state, base_ref, weight_ref, out_ref):
    comps, rows, cols = state.shape
    half = cols // 2
    flat = state.reshape(comps * rows, cols)
    stacked = jnp.concatenate(split(flat), axis=0)
    at = lax.broadcasted_iota(jnp.int32, (cols, cols), 0)
    to = lax.broadcasted_iota(jnp.int32, (cols, cols), 1)
    source_col = jnp.where(to < half, 2 * to, 2 * (to - half) + 1)
    order = jnp.where(at == source_col, 1.0, 0.0).astype(BF16)
    ordered = jnp.dot(stacked, order, preferred_element_type=F32).astype(BF16)
    even, odd = ordered[:, :half], ordered[:, half:]
    blocks, slots = base_ref.shape
    row_iota = lax.broadcasted_iota(jnp.int32, (rows, slots), 0)

    def one(d):
        base = base_ref[pl.ds(d, 1), :]
        w0 = weight_ref[0, pl.ds(d, 1), :]
        w1 = weight_ref[1, pl.ds(d, 1), :]
        w2 = weight_ref[2, pl.ds(d, 1), :]
        w3 = weight_ref[3, pl.ds(d, 1), :]
        row, col = divmod_const(base, cols)
        is_odd = (col & 1) == 1
        wraps = col == cols - 1
        odd_at = col >> 1
        even_at = jnp.where(wraps, 0, (col + 1) >> 1)
        even_row = row + jnp.where(wraps, 1, 0)
        picked_even = jnp.dot(even, one_hot(even_at, half), preferred_element_type=F32)
        picked_odd = jnp.dot(odd, one_hot(odd_at, half), preferred_element_type=F32)
        count = comps * rows
        picked_even = (picked_even[:count] + picked_even[count:]).reshape(comps, rows, slots)
        picked_odd = (picked_odd[:count] + picked_odd[count:]).reshape(comps, rows, slots)
        even_weight = jnp.where(
            row_iota == even_row,
            jnp.where(is_odd, w1, w0),
            jnp.where(row_iota == even_row + 1, jnp.where(is_odd, w3, w2), 0.0),
        )
        odd_weight = jnp.where(
            row_iota == row,
            jnp.where(is_odd, w0, w1),
            jnp.where(row_iota == row + 1, jnp.where(is_odd, w2, w3), 0.0),
        )
        total = even_weight[None] * picked_even + odd_weight[None] * picked_odd
        out_ref[d, 0:comps, :] = jnp.sum(total, axis=1)

    repeat(blocks, one)
    none = jnp.zeros((comps, slots), F32)
    for d in range(blocks):
        out_ref[d, comps : 2 * comps, :] = out_ref[d - 1, 0:comps, :] if d > 0 else none
        out_ref[d, 2 * comps : 3 * comps, :] = out_ref[d + 1, 0:comps, :] if d < blocks - 1 else none


def selected(hit, values):
    count = values.shape[0] * hit.shape[0]
    parts = [
        jnp.where(hit[None], part.astype(F32)[:, None, :], 0.0).reshape(count, -1).astype(BF16)
        for part in split(values)
    ]
    return jnp.concatenate(parts, axis=0)


def add_product(acc_ref, left, right):
    out = lax.dot_general(left, right, (((1,), (1,)), ((), ())), preferred_element_type=F32)
    count = acc_ref.shape[0]
    acc_ref[...] += out if left.shape[0] == count else out[:count] + out[count:]


def frozen_count(target_ref, rows, cols, acc_ref):
    blocks, slots = target_ref.shape
    row_iota = lax.broadcasted_iota(jnp.int32, (rows, slots), 0)
    acc_ref[...] = jnp.zeros_like(acc_ref)

    def one(b):
        row, col = divmod_const(target_ref[pl.ds(b, 1), :], cols)
        add_product(acc_ref, jnp.where(row_iota == row, 1.0, 0.0).astype(BF16), one_hot(col, cols))

    repeat(blocks, one, 4)


def place_own(arrived_ref, target_ref, comps, rows, cols, acc_ref):
    blocks, slots = target_ref.shape
    row_iota = lax.broadcasted_iota(jnp.int32, (rows, slots), 0)
    acc_ref[...] = jnp.zeros_like(acc_ref)

    def one(b):
        row, col = divmod_const(target_ref[pl.ds(b, 1), :], cols)
        left = selected(row_iota == row, arrived_ref[b, 0:comps, :])
        add_product(acc_ref, left, one_hot(col, cols))

    repeat(blocks, one)


def place_halo(arrived_ref, first, target_ref, start, comps, cols, acc_ref, out_ref):
    blocks, slots = target_ref.shape
    tiles = cols // LANES
    group = ROWS // 2
    row_iota = lax.broadcasted_iota(jnp.int32, (tiles * group, slots), 0)
    acc_ref[...] = jnp.zeros_like(acc_ref)

    def one(b):
        row, col = divmod_const(target_ref[pl.ds(b, 1), :], cols)
        row = row - start
        hit = row_iota == (col >> LANE_BITS) * group + (row & (group - 1))
        at = (row >> GROUP_BITS) * LANES + (col & (LANES - 1))
        left = selected(hit, arrived_ref[b, first : first + comps, :])
        add_product(acc_ref, left, one_hot(at, 2 * LANES))

    repeat(blocks, one)
    for c in range(comps):
        for t in range(tiles):
            for h in range(2):
                out_ref[c, h * group : (h + 1) * group, t * LANES : (t + 1) * LANES] = acc_ref[
                    (c * tiles + t) * group : (c * tiles + t + 1) * group,
                    h * LANES : (h + 1) * LANES,
                ]


def border_rows(state_ref, movable_ref, top_ref, bottom_ref):
    comps, rows, _ = state_ref.shape
    upper = movable_ref[rows - ROWS :, :] > 0.5
    lower = movable_ref[:ROWS, :] > 0.5
    for c in range(comps):
        kept = jnp.where(upper, state_ref[c, rows - ROWS :, :], 0.0)
        top_ref[c * LOW : (c + 1) * LOW, :] = kept[ROWS - LOW :, :]
        kept = jnp.where(lower, state_ref[c, :ROWS, :], 0.0)
        bottom_ref[c * HIGH : (c + 1) * HIGH, :] = kept[:HIGH, :]


def start_kernel(
    field_hbm, base_hbm, weight_hbm, target_hbm, source_hbm, inverse_hbm, coupling_hbm,
    sums_ref, movable_ref, top_ref, bottom_ref,
    field_ref, base_ref, weight_ref, target_ref, source_ref, inverse_ref, coupling_ref, acc_ref, sems,
):
    comps, rows, cols = field_ref.shape
    blocks, slots = target_ref.shape
    last = slice(rows - ROWS, rows)
    first = slice(0, ROWS)
    copies = [
        (target_hbm, target_ref),
        (field_hbm, field_ref),
        (base_hbm, base_ref),
        (weight_hbm, weight_ref),
        (source_hbm.at[:, last], source_ref.at[0]),
        (source_hbm.at[:, first], source_ref.at[1]),
        (inverse_hbm.at[:, :, last], inverse_ref.at[0]),
        (inverse_hbm.at[:, :, first], inverse_ref.at[1]),
        (coupling_hbm.at[:, last], coupling_ref.at[0]),
        (coupling_hbm.at[:, first], coupling_ref.at[1]),
    ]
    copies = [pltpu.make_async_copy(a, b, sems.at[i]) for i, (a, b) in enumerate(copies)]
    for copy in copies:
        copy.start()
    copies[0].wait()
    frozen_count(target_ref, rows, cols, acc_ref)
    movable_ref[...] = jnp.where(acc_ref[...] > 0.5, 0.0, 1.0)
    for copy in copies[1:4]:
        copy.wait()
    donor_sums(field_ref[...], base_ref, weight_ref, sums_ref)
    border_rows(field_ref, movable_ref, top_ref, bottom_ref)
    for copy in copies[4:]:
        copy.wait()
    sides = (
        (top_ref, 0, comps * LOW, LOW_DONE, ROWS - LOW_DONE, rows - ROWS),
        (bottom_ref, 1, comps * HIGH, HIGH_DONE, 0, 0),
    )
    for ref, side, offset, count, at, movable_at in sides:
        fixed = [inverse_ref[side, v, w] for v in range(comps) for w in range(comps)]
        fixed += [source_ref[side, w] for w in range(comps)]
        fixed += [coupling_ref[side, i] for i in range(coupling_ref.shape[1])]
        fixed.append(movable_ref[movable_at : movable_at + ROWS, :])
        for value in fixed:
            ref[offset : offset + count, :] = value[at : at + count, :]
            offset += count
        per = cols // slots
        deep = blocks // per
        for i in range(per):
            cells = target_ref[i * deep : (i + 1) * deep, :].astype(F32)
            ref[offset : offset + deep, i * slots : (i + 1) * slots] = cells


def unpack_kernel(
    top_ref, bottom_ref, low_ref, high_ref, low_target_ref, high_target_ref, *, comps
):
    sides = (
        (top_ref, comps * LOW, LOW_DONE, ROWS - LOW_DONE, low_ref, low_target_ref),
        (bottom_ref, comps * HIGH, HIGH_DONE, 0, high_ref, high_target_ref),
    )
    for ref, offset, count, at, out_ref, target_ref in sides:
        cols = ref.shape[1]
        blocks, slots = target_ref.shape
        for i in range(out_ref.shape[0]):
            out_ref[i] = jnp.zeros((ROWS, cols), F32)
            out_ref[i, at : at + count, :] = ref[offset : offset + count, :]
            offset += count
        per = cols // slots
        deep = blocks // per
        for i in range(per):
            cells = ref[offset : offset + deep, i * slots : (i + 1) * slots]
            target_ref[i * deep : (i + 1) * deep, :] = cells.astype(jnp.int32)


def place(
    arrived_ref, target_ref, state_ref, movable_ref, low_target_ref, high_target_ref,
    out_ref, below_ref, above_ref, acc_ref, halo_ref,
):
    comps, rows, cols = state_ref.shape
    place_own(arrived_ref, target_ref, comps, rows, cols, acc_ref)
    movable = movable_ref[...] > 0.5
    for c in range(comps):
        out_ref[c] = jnp.where(movable, state_ref[c], acc_ref[c * rows : (c + 1) * rows, :])
    place_halo(arrived_ref, comps, low_target_ref, rows - ROWS, comps, cols, halo_ref, below_ref)
    place_halo(arrived_ref, 2 * comps, high_target_ref, 0, comps, cols, halo_ref, above_ref)


def sections(u_ref, start, parts, write, is_near, parity, comps, cols):
    source, inverse, coupling, movable = parts
    lanes = lax.broadcasted_iota(jnp.int32, (ROWS, cols), 1)
    sublanes = lax.broadcasted_iota(jnp.int32, (ROWS, cols), 0)

    def rows_at(c, offset):
        return u_ref[c, start + offset : start + offset + ROWS, :]

    def shifted(value, offset):
        return pltpu.roll(value, (-offset) % cols, 1)

    def finish(update, terms, mask):
        for v in range(comps):
            total = update(v)
            for w in range(comps):
                product = inverse(v, w) * terms[w]
                total = product if total is None else total + product
            write(v, jnp.where(mask, total, rows_at(v, 0)))

    @pl.when(is_near)
    def _():
        c0, c1, c2, c3 = (coupling(i) for i in range(4))
        c2 = jnp.where(lanes >= 1, c2, 0.0)
        c3 = jnp.where(lanes < cols - 1, c3, 0.0)
        terms = []
        for w in range(comps):
            here = rows_at(w, 0)
            term = source(w) + c0 * rows_at(w, -1) + c1 * rows_at(w, 1)
            terms.append(term + c2 * shifted(here, -1) + c3 * shifted(here, 1))
        colour = ((lanes + sublanes) & 1) == parity
        finish(lambda v: None, terms, colour & (movable() > 0.5))

    @pl.when(jnp.logical_not(is_near))
    def _():
        c0, c1 = coupling(0), coupling(1)
        factors = []
        for offset, weight in zip(upwind_offsets, upwind_weights):
            inside = (lanes + offset >= 0) & (lanes + offset < cols)
            factors.append(weight if offset == 0 else jnp.where(inside, weight, 0.0))
        terms = []
        for w in range(comps):
            here = rows_at(w, 0)
            along_j = along_k = None
            for offset, weight, factor in zip(upwind_offsets, upwind_weights, factors):
                in_j = weight * rows_at(w, offset)
                in_k = factor * (here if offset == 0 else shifted(here, offset))
                along_j = in_j if along_j is None else along_j + in_j
                along_k = in_k if along_k is None else along_k + in_k
            terms.append(source(w) - c0 * along_j - c1 * along_k)
        finish(lambda v: rows_at(v, 0), terms, movable() > 0.5)


def sweep(state_ref, below_ref, above_ref, placed_below_ref, placed_above_ref, movable_ref, work, out_ref):
    comps, rows, cols = state_ref.shape
    source_ref, inverse_ref, coupling_ref = work["source"], work["inverse"], work["coupling"]
    low_ref, high_ref, u_ref, v_ref = work["low"], work["high"], work["u"], work["v"]
    is_near = lax.axis_index("group") == 0
    for c in range(comps):
        u_ref[c, PAD : PAD + rows, :] = state_ref[c]
        u_ref[c, PAD - LOW : PAD, :] = (
            below_ref[c * LOW : (c + 1) * LOW, :] + placed_below_ref[c, ROWS - LOW :, :]
        )
        u_ref[c, PAD + rows : PAD + rows + HIGH, :] = (
            above_ref[c * HIGH : (c + 1) * HIGH, :] + placed_above_ref[c, :HIGH, :]
        )

    def own(r):
        at = slice(r, r + ROWS)
        return (
            lambda w: source_ref[w, at, :],
            lambda v, w: inverse_ref[v, w, at, :],
            lambda i: coupling_ref[i, at, :],
            lambda: movable_ref[at, :],
        )

    def packed(ref):
        first = comps * comps
        second = first + comps
        last = ref.shape[0] - 1
        return (
            lambda w: ref[first + w],
            lambda v, w: ref[v * comps + w],
            lambda i: ref[second + i],
            lambda: ref[last],
        )

    def into(ref, start):
        def write(v, value):
            ref[v, start : start + ROWS, :] = value

        return write

    wait = work["wait"]
    for r in range(0, rows, ROWS):
        wait(r)
        sections(u_ref, PAD + r, own(r), into(v_ref, PAD + r), is_near, 0, comps, cols)
    wait("low")
    sections(u_ref, PAD - ROWS, packed(low_ref), into(v_ref, PAD - ROWS), is_near, 0, comps, cols)
    wait("high")
    sections(u_ref, PAD + rows, packed(high_ref), into(v_ref, PAD + rows), is_near, 0, comps, cols)
    for r in range(0, rows, ROWS):
        sections(v_ref, PAD + r, own(r), into(out_ref, r), is_near, 1, comps, cols)


def step_kernel(names, is_last, refs):
    refs = list(refs)
    operands, refs = refs[:6], refs[6:]
    held, refs = refs[: len(names)], refs[len(names) :]
    out_ref = refs.pop(0)
    if not is_last:
        sums_ref, top_ref, bottom_ref = refs[:3]
        refs = refs[3:]
    copied, (u_ref, v_ref, sems) = refs[: len(names)], refs[len(names) :]
    rows = out_ref.shape[1]
    work = dict(zip(names, copied))
    work.update(u=u_ref, v=v_ref)
    copies = {}
    count = 0

    def copy(key, source, target):
        nonlocal count
        copies.setdefault(key, []).append(pltpu.make_async_copy(source, target, sems.at[count]))
        count += 1

    whole = dict(zip(names, held))
    for r in range(0, rows, ROWS):
        at = slice(r, r + ROWS)
        copy(r, whole["inverse"].at[:, :, at], work["inverse"].at[:, :, at])
        copy(r, whole["source"].at[:, at], work["source"].at[:, at])
        copy(r, whole["coupling"].at[:, at], work["coupling"].at[:, at])
    for name in names:
        if name not in ("inverse", "source", "coupling"):
            copy(name, whole[name], work[name])
    for group in copies.values():
        for one in group:
            one.start()

    def wait(key):
        for one in copies[key]:
            one.wait()

    work["wait"] = wait
    sweep(*operands, work, out_ref)
    if not is_last:
        movable_ref = operands[5]
        border_rows(out_ref, movable_ref, top_ref, bottom_ref)
        wait("base")
        wait("weight")
        donor_sums(out_ref[...], work["base"], work["weight"], sums_ref)


def on_device(field, source, block_inverse, coupling, donor_base, donor_weight, receiver_cell):
    state = field[0, 0]
    source = source[0, 0]
    inverse = block_inverse[0, 0]
    coupling = coupling[0, 0]
    base = donor_base[0, 0]
    weight = donor_weight[0, 0]
    target = receiver_cell[0, 0]
    comps, rows, cols = state.shape
    faces = coupling.shape[0]
    blocks, slots = base.shape
    groups = lax.axis_size("group")
    swap = [(g * blocks + b, (groups - 1 - g) * blocks + b) for g in range(groups) for b in range(blocks)]
    up = [(b, b + 1) for b in range(blocks - 1)]
    down = [(b + 1, b) for b in range(blocks - 1)]

    def f32(*shape):
        return jax.ShapeDtypeStruct(shape, F32)

    def call(kernel, operands, remote, outs, scratch):
        remote = [pltpu.with_memory_space_constraint(value, pltpu.HBM) for value in remote]
        return pl.pallas_call(
            kernel,
            out_shape=outs,
            in_specs=vmem(len(operands)) + [pl.BlockSpec(memory_space=pltpu.HBM)] * len(remote),
            out_specs=tuple(vmem(len(outs))),
            scratch_shapes=scratch,
            compiler_params=pltpu.CompilerParams(vmem_limit_bytes=VMEM_LIMIT),
        )(*operands, *remote)

    def vmem_like(*shape, dtype=F32):
        return pltpu.VMEM(shape, dtype)

    fixed = comps * comps + comps + faces + 1
    cells = f32(comps, rows, cols)
    sums_shape = f32(blocks, -(-3 * comps // ROWS) * ROWS, slots)
    deep = blocks * slots // cols

    sums, movable, top, bottom = call(
        start_kernel,
        (),
        (state, base, weight, target, source, inverse, coupling),
        (
            sums_shape,
            f32(rows, cols),
            f32(comps * LOW + fixed * LOW_DONE + deep, cols),
            f32(comps * HIGH + fixed * HIGH_DONE + deep, cols),
        ),
        [
            vmem_like(comps, rows, cols),
            vmem_like(blocks, slots, dtype=jnp.int32),
            vmem_like(*weight.shape),
            vmem_like(blocks, slots, dtype=jnp.int32),
            vmem_like(2, comps, ROWS, cols),
            vmem_like(2, comps, comps, ROWS, cols),
            vmem_like(2, faces, ROWS, cols),
            vmem_like(rows, cols),
            pltpu.SemaphoreType.DMA((10,)),
        ],
    )

    placing = [vmem_like(comps * rows, cols), vmem_like(comps * (cols // LANES) * (ROWS // 2), 2 * LANES)]
    working = [vmem_like(comps, rows + 2 * PAD, cols)] * 2
    held = {"source": source, "inverse": inverse, "coupling": coupling, "base": base, "weight": weight}
    border = (f32(comps * LOW, cols), f32(comps * HIGH, cols))
    halo = f32(comps, ROWS, cols)
    for iteration in range(ITERS):
        arrived = lax.ppermute(sums, ("group", "blk"), swap)
        arrived = lax.all_to_all(arrived, "blk", split_axis=0, concat_axis=0, tiled=True)
        below = lax.ppermute(top, "blk", up)
        above = lax.ppermute(bottom, "blk", down)
        is_last = iteration == ITERS - 1
        if iteration == 0:
            cells_of = jax.ShapeDtypeStruct((blocks, slots), jnp.int32)
            held["low"], held["high"], low_target, high_target = call(
                partial(unpack_kernel, comps=comps),
                (below, above),
                (),
                (f32(fixed, ROWS, cols), f32(fixed, ROWS, cols), cells_of, cells_of),
                [],
            )
        state, placed_below, placed_above = call(
            place,
            (arrived, target, state, movable, low_target, high_target),
            (),
            (cells, halo, halo),
            placing,
        )
        names = tuple(name for name in held if not (is_last and name in ("base", "weight")))
        copied = [vmem_like(*held[name].shape, dtype=held[name].dtype) for name in names]
        results = call(
            lambda *refs: step_kernel(names, is_last, refs),
            (state, below, above, placed_below, placed_above, movable),
            tuple(held[name] for name in names),
            (cells,) if is_last else (cells, sums_shape, *border),
            copied + working + [pltpu.SemaphoreType.DMA((3 * (rows // ROWS) + len(names),))],
        )
        state = results[0]
        if not is_last:
            sums, top, bottom = results[1:]
    return state[None, None]


def solution(mesh):
    in_specs = (
        P("group", "blk", None, None, None),
        P("group", "blk", None, None, None),
        P("group", "blk", None, None, None, None),
        P("group", "blk", None, None, None),
        P("group", "blk", None, None),
        P("group", "blk", None, None, None),
        P("group", "blk", None, None),
    )
    out_specs = P("group", "blk", None, None, None)
    return jax.shard_map(
        on_device, mesh=mesh, in_specs=in_specs, out_specs=out_specs, check_vma=False
    )
```

```python
from functools import partial

import jax
import jax.numpy as jnp
from jax import lax
from jax.experimental import pallas as pl
from jax.experimental.pallas import tpu as pltpu
from jax.sharding import PartitionSpec as P


ITERS = 4

upwind_offsets = (-3, -2, -1, 0, 1, 2)
upwind_weights = (-2.0 / 60.0, 15.0 / 60.0, -60.0 / 60.0, 20.0 / 60.0, 30.0 / 60.0, -3.0 / 60.0)

F32 = jnp.float32
BF16 = jnp.bfloat16
ROWS = 8
LOW, HIGH = 6, 4
LOW_DONE, HIGH_DONE = 3, 2
PAD = 2 * ROWS
LANES, LANE_BITS, GROUP_BITS = 128, 7, 2
UNROLL = 16
VMEM_LIMIT = 16 * 1024 * 1024


def vmem(count):
    return [pl.BlockSpec(memory_space=pltpu.VMEM)] * count


def divmod_const(value, size):
    if size & (size - 1) == 0:
        return value >> (size.bit_length() - 1), value & (size - 1)
    quotient = lax.div(value, jnp.int32(size))
    return quotient, value - quotient * size


def one_hot(index, size):
    rows = lax.broadcasted_iota(jnp.int32, (size, index.shape[1]), 0)
    return jnp.where(rows == index, 1.0, 0.0).astype(BF16)


def split(value):
    high = value.astype(BF16)
    low = (value - high.astype(F32)).astype(BF16)
    return high, low


def repeat(count, step, unroll=UNROLL):
    lax.fori_loop(0, count, lambda i, carry: (step(i), carry)[1], 0, unroll=min(count, unroll))


def donor_sums(state, base_ref, weight_ref, out_ref):
    comps, rows, cols = state.shape
    half = cols // 2
    flat = state.reshape(comps * rows, cols)
    stacked = jnp.concatenate(split(flat), axis=0)
    at = lax.broadcasted_iota(jnp.int32, (cols, cols), 0)
    to = lax.broadcasted_iota(jnp.int32, (cols, cols), 1)
    source_col = jnp.where(to < half, 2 * to, 2 * (to - half) + 1)
    order = jnp.where(at == source_col, 1.0, 0.0).astype(BF16)
    ordered = jnp.dot(stacked, order, preferred_element_type=F32).astype(BF16)
    even, odd = ordered[:, :half], ordered[:, half:]
    blocks, slots = base_ref.shape
    row_iota = lax.broadcasted_iota(jnp.int32, (rows, slots), 0)

    def one(d):
        base = base_ref[pl.ds(d, 1), :]
        w0 = weight_ref[0, pl.ds(d, 1), :]
        w1 = weight_ref[1, pl.ds(d, 1), :]
        w2 = weight_ref[2, pl.ds(d, 1), :]
        w3 = weight_ref[3, pl.ds(d, 1), :]
        row, col = divmod_const(base, cols)
        is_odd = (col & 1) == 1
        wraps = col == cols - 1
        odd_at = col >> 1
        even_at = jnp.where(wraps, 0, (col + 1) >> 1)
        even_row = row + jnp.where(wraps, 1, 0)
        picked_even = jnp.dot(even, one_hot(even_at, half), preferred_element_type=F32)
        picked_odd = jnp.dot(odd, one_hot(odd_at, half), preferred_element_type=F32)
        count = comps * rows
        picked_even = (picked_even[:count] + picked_even[count:]).reshape(comps, rows, slots)
        picked_odd = (picked_odd[:count] + picked_odd[count:]).reshape(comps, rows, slots)
        even_weight = jnp.where(
            row_iota == even_row,
            jnp.where(is_odd, w1, w0),
            jnp.where(row_iota == even_row + 1, jnp.where(is_odd, w3, w2), 0.0),
        )
        odd_weight = jnp.where(
            row_iota == row,
            jnp.where(is_odd, w0, w1),
            jnp.where(row_iota == row + 1, jnp.where(is_odd, w2, w3), 0.0),
        )
        total = even_weight[None] * picked_even + odd_weight[None] * picked_odd
        out_ref[d, 0:comps, :] = jnp.sum(total, axis=1)

    repeat(blocks, one)
    none = jnp.zeros((comps, slots), F32)
    for d in range(blocks):
        out_ref[d, comps : 2 * comps, :] = out_ref[d - 1, 0:comps, :] if d > 0 else none
        out_ref[d, 2 * comps : 3 * comps, :] = out_ref[d + 1, 0:comps, :] if d < blocks - 1 else none


def selected(hit, values):
    count = values.shape[0] * hit.shape[0]
    parts = [
        jnp.where(hit[None], part.astype(F32)[:, None, :], 0.0).reshape(count, -1).astype(BF16)
        for part in split(values)
    ]
    return jnp.concatenate(parts, axis=0)


def add_product(acc_ref, left, right):
    out = lax.dot_general(left, right, (((1,), (1,)), ((), ())), preferred_element_type=F32)
    count = acc_ref.shape[0]
    acc_ref[...] += out if left.shape[0] == count else out[:count] + out[count:]


def frozen_kernel(target_ref, movable_ref, acc_ref):
    rows, cols = movable_ref.shape
    blocks, slots = target_ref.shape
    row_iota = lax.broadcasted_iota(jnp.int32, (rows, slots), 0)
    acc_ref[...] = jnp.zeros_like(acc_ref)

    def one(b):
        row, col = divmod_const(target_ref[pl.ds(b, 1), :], cols)
        add_product(acc_ref, jnp.where(row_iota == row, 1.0, 0.0).astype(BF16), one_hot(col, cols))

    repeat(blocks, one, 4)
    movable_ref[...] = jnp.where(acc_ref[...] > 0.5, 0.0, 1.0)


def place_own(arrived_ref, target_ref, comps, rows, cols, acc_ref):
    blocks, slots = target_ref.shape
    row_iota = lax.broadcasted_iota(jnp.int32, (rows, slots), 0)
    acc_ref[...] = jnp.zeros_like(acc_ref)

    def one(b):
        row, col = divmod_const(target_ref[pl.ds(b, 1), :], cols)
        left = selected(row_iota == row, arrived_ref[b, 0:comps, :])
        add_product(acc_ref, left, one_hot(col, cols))

    repeat(blocks, one)


def place_halo(arrived_ref, first, target_ref, start, comps, cols, acc_ref, out_ref, unroll=UNROLL):
    blocks, slots = target_ref.shape
    tiles = cols // LANES
    group = ROWS // 2
    row_iota = lax.broadcasted_iota(jnp.int32, (tiles * group, slots), 0)
    acc_ref[...] = jnp.zeros_like(acc_ref)

    def one(b):
        row, col = divmod_const(target_ref[pl.ds(b, 1), :], cols)
        row = row - start
        hit = row_iota == (col >> LANE_BITS) * group + (row & (group - 1))
        at = (row >> GROUP_BITS) * LANES + (col & (LANES - 1))
        if arrived_ref is None:
            left = jnp.where(hit, 1.0, 0.0).astype(BF16)
        else:
            left = selected(hit, arrived_ref[b, first : first + comps, :])
        add_product(acc_ref, left, one_hot(at, 2 * LANES))

    repeat(blocks, one, unroll)
    for c in range(comps):
        for t in range(tiles):
            for h in range(2):
                out_ref[c, h * group : (h + 1) * group, t * LANES : (t + 1) * LANES] = acc_ref[
                    (c * tiles + t) * group : (c * tiles + t + 1) * group,
                    h * LANES : (h + 1) * LANES,
                ]


def border_rows(state_ref, movable_ref, top_ref, bottom_ref):
    comps, rows, _ = state_ref.shape
    upper = movable_ref[rows - ROWS :, :] > 0.5
    lower = movable_ref[:ROWS, :] > 0.5
    for c in range(comps):
        kept = jnp.where(upper, state_ref[c, rows - ROWS :, :], 0.0)
        top_ref[c * LOW : (c + 1) * LOW, :] = kept[ROWS - LOW :, :]
        kept = jnp.where(lower, state_ref[c, :ROWS, :], 0.0)
        bottom_ref[c * HIGH : (c + 1) * HIGH, :] = kept[:HIGH, :]


def start_kernel(
    field_hbm, base_hbm, weight_hbm, target_hbm, source_hbm, inverse_hbm, coupling_hbm,
    sums_ref, top_ref, bottom_ref,
    field_ref, base_ref, weight_ref, target_ref, source_ref, inverse_ref, coupling_ref, sems,
):
    comps, rows, cols = field_ref.shape
    blocks, slots = target_ref.shape
    last = slice(rows - ROWS, rows)
    first = slice(0, ROWS)
    copies = [
        (field_hbm, field_ref),
        (base_hbm, base_ref),
        (weight_hbm, weight_ref),
        (target_hbm, target_ref),
        (source_hbm.at[:, last], source_ref.at[0]),
        (source_hbm.at[:, first], source_ref.at[1]),
        (inverse_hbm.at[:, :, last], inverse_ref.at[0]),
        (inverse_hbm.at[:, :, first], inverse_ref.at[1]),
        (coupling_hbm.at[:, last], coupling_ref.at[0]),
        (coupling_hbm.at[:, first], coupling_ref.at[1]),
    ]
    copies = [pltpu.make_async_copy(a, b, sems.at[i]) for i, (a, b) in enumerate(copies)]
    for copy in copies:
        copy.start()
    for copy in copies[:3]:
        copy.wait()
    donor_sums(field_ref[...], base_ref, weight_ref, sums_ref)
    for c in range(comps):
        top_ref[c * LOW : (c + 1) * LOW, :] = field_ref[c, rows - LOW :, :]
        bottom_ref[c * HIGH : (c + 1) * HIGH, :] = field_ref[c, :HIGH, :]
    for copy in copies[3:]:
        copy.wait()
    sides = (
        (top_ref, 0, comps * LOW, LOW_DONE, ROWS - LOW_DONE),
        (bottom_ref, 1, comps * HIGH, HIGH_DONE, 0),
    )
    for ref, side, offset, count, at in sides:
        fixed = [inverse_ref[side, v, w] for v in range(comps) for w in range(comps)]
        fixed += [source_ref[side, w] for w in range(comps)]
        fixed += [coupling_ref[side, i] for i in range(coupling_ref.shape[1])]
        for value in fixed:
            ref[offset : offset + count, :] = value[at : at + count, :]
            offset += count
        per = cols // slots
        deep = blocks // per
        for i in range(per):
            cells = target_ref[i * deep : (i + 1) * deep, :].astype(F32)
            ref[offset : offset + deep, i * slots : (i + 1) * slots] = cells


def unpack_kernel(
    top_ref, bottom_ref, low_ref, high_ref, low_target_ref, high_target_ref, below_ref, above_ref,
    acc_ref, count_ref, *, comps, rows,
):
    cols = top_ref.shape[1]
    sublanes = lax.broadcasted_iota(jnp.int32, (ROWS, cols), 0)
    sides = (
        (top_ref, LOW, LOW_DONE, ROWS - LOW, ROWS - LOW_DONE, rows - ROWS, low_ref, low_target_ref, below_ref),
        (bottom_ref, HIGH, HIGH_DONE, 0, 0, 0, high_ref, high_target_ref, above_ref),
    )
    for ref, wide, count, wide_at, at, start, out_ref, target_ref, halo_ref in sides:
        blocks, slots = target_ref.shape
        offset = comps * wide
        last = out_ref.shape[0] - 1
        for i in range(last):
            out_ref[i] = jnp.zeros((ROWS, cols), F32)
            out_ref[i, at : at + count, :] = ref[offset : offset + count, :]
            offset += count
        per = cols // slots
        deep = blocks // per
        for i in range(per):
            cells = ref[offset : offset + deep, i * slots : (i + 1) * slots]
            target_ref[i * deep : (i + 1) * deep, :] = cells.astype(jnp.int32)
        place_halo(None, 0, target_ref, start, 1, cols, acc_ref, count_ref, 4)
        movable = count_ref[0] < 0.5
        done = (sublanes >= at) & (sublanes < at + count)
        out_ref[last] = jnp.where(movable & done, 1.0, 0.0)
        movable = count_ref[0, wide_at : wide_at + wide, :] < 0.5
        for c in range(comps):
            halo_ref[c * wide : (c + 1) * wide, :] = jnp.where(
                movable, ref[c * wide : (c + 1) * wide, :], 0.0
            )


def place(
    arrived_ref, target_ref, state_ref, movable_ref, low_target_ref, high_target_ref,
    out_ref, below_ref, above_ref, acc_ref, halo_ref,
):
    comps, rows, cols = state_ref.shape
    place_own(arrived_ref, target_ref, comps, rows, cols, acc_ref)
    movable = movable_ref[...] > 0.5
    for c in range(comps):
        out_ref[c] = jnp.where(movable, state_ref[c], acc_ref[c * rows : (c + 1) * rows, :])
    place_halo(arrived_ref, comps, low_target_ref, rows - ROWS, comps, cols, halo_ref, below_ref)
    place_halo(arrived_ref, 2 * comps, high_target_ref, 0, comps, cols, halo_ref, above_ref)


def sections(u_ref, start, parts, write, is_near, parity, comps, cols):
    source, inverse, coupling, movable = parts
    lanes = lax.broadcasted_iota(jnp.int32, (ROWS, cols), 1)
    sublanes = lax.broadcasted_iota(jnp.int32, (ROWS, cols), 0)

    def rows_at(c, offset):
        return u_ref[c, start + offset : start + offset + ROWS, :]

    def shifted(value, offset):
        return pltpu.roll(value, (-offset) % cols, 1)

    def finish(update, terms, mask):
        for v in range(comps):
            total = update(v)
            for w in range(comps):
                product = inverse(v, w) * terms[w]
                total = product if total is None else total + product
            write(v, jnp.where(mask, total, rows_at(v, 0)))

    @pl.when(is_near)
    def _():
        c0, c1, c2, c3 = (coupling(i) for i in range(4))
        c2 = jnp.where(lanes >= 1, c2, 0.0)
        c3 = jnp.where(lanes < cols - 1, c3, 0.0)
        terms = []
        for w in range(comps):
            here = rows_at(w, 0)
            term = source(w) + c0 * rows_at(w, -1) + c1 * rows_at(w, 1)
            terms.append(term + c2 * shifted(here, -1) + c3 * shifted(here, 1))
        colour = ((lanes + sublanes) & 1) == parity
        finish(lambda v: None, terms, colour & (movable() > 0.5))

    @pl.when(jnp.logical_not(is_near))
    def _():
        c0, c1 = coupling(0), coupling(1)
        factors = []
        for offset, weight in zip(upwind_offsets, upwind_weights):
            inside = (lanes + offset >= 0) & (lanes + offset < cols)
            factors.append(weight if offset == 0 else jnp.where(inside, weight, 0.0))
        terms = []
        for w in range(comps):
            here = rows_at(w, 0)
            along_j = along_k = None
            for offset, weight, factor in zip(upwind_offsets, upwind_weights, factors):
                in_j = weight * rows_at(w, offset)
                in_k = factor * (here if offset == 0 else shifted(here, offset))
                along_j = in_j if along_j is None else along_j + in_j
                along_k = in_k if along_k is None else along_k + in_k
            terms.append(source(w) - c0 * along_j - c1 * along_k)
        finish(lambda v: rows_at(v, 0), terms, movable() > 0.5)


def sweep(state_ref, below_ref, above_ref, placed_below_ref, placed_above_ref, movable_ref, work, out_ref):
    comps, rows, cols = state_ref.shape
    source_ref, inverse_ref, coupling_ref = work["source"], work["inverse"], work["coupling"]
    low_ref, high_ref, u_ref, v_ref = work["low"], work["high"], work["u"], work["v"]
    is_near = lax.axis_index("group") == 0
    for c in range(comps):
        u_ref[c, PAD : PAD + rows, :] = state_ref[c]
        u_ref[c, PAD - LOW : PAD, :] = (
            below_ref[c * LOW : (c + 1) * LOW, :] + placed_below_ref[c, ROWS - LOW :, :]
        )
        u_ref[c, PAD + rows : PAD + rows + HIGH, :] = (
            above_ref[c * HIGH : (c + 1) * HIGH, :] + placed_above_ref[c, :HIGH, :]
        )

    def own(r):
        at = slice(r, r + ROWS)
        return (
            lambda w: source_ref[w, at, :],
            lambda v, w: inverse_ref[v, w, at, :],
            lambda i: coupling_ref[i, at, :],
            lambda: movable_ref[at, :],
        )

    def packed(ref):
        first = comps * comps
        second = first + comps
        last = ref.shape[0] - 1
        return (
            lambda w: ref[first + w],
            lambda v, w: ref[v * comps + w],
            lambda i: ref[second + i],
            lambda: ref[last],
        )

    def into(ref, start):
        def write(v, value):
            ref[v, start : start + ROWS, :] = value

        return write

    for r in range(0, rows, ROWS):
        sections(u_ref, PAD + r, own(r), into(v_ref, PAD + r), is_near, 0, comps, cols)
    sections(u_ref, PAD - ROWS, packed(low_ref), into(v_ref, PAD - ROWS), is_near, 0, comps, cols)
    sections(u_ref, PAD + rows, packed(high_ref), into(v_ref, PAD + rows), is_near, 0, comps, cols)
    for r in range(0, rows, ROWS):
        sections(v_ref, PAD + r, own(r), into(out_ref, r), is_near, 1, comps, cols)


def place_kernel(count, refs):
    refs = list(refs)
    operands, refs = refs[:6], refs[6:]
    held, refs = refs[:count], refs[count:]
    results, refs = refs[:3], refs[3:]
    copied, (acc_ref, halo_ref, sems) = refs[:count], refs[count:]
    copies = [pltpu.make_async_copy(held[i], copied[i], sems.at[i]) for i in range(count)]
    for copy in copies:
        copy.start()
    place(*operands, *results, acc_ref, halo_ref)
    for copy in copies:
        copy.wait()


def step_kernel(names, is_last, refs):
    refs = list(refs)
    operands, refs = refs[:6], refs[6:]
    work, refs = dict(zip(names, refs)), refs[len(names) :]
    out_ref = refs.pop(0)
    if not is_last:
        sums_ref, top_ref, bottom_ref = refs[:3]
        refs = refs[3:]
    work["u"], work["v"] = refs
    sweep(*operands, work, out_ref)
    if not is_last:
        border_rows(out_ref, operands[5], top_ref, bottom_ref)
        donor_sums(out_ref[...], work["base"], work["weight"], sums_ref)


def on_device(field, source, block_inverse, coupling, donor_base, donor_weight, receiver_cell):
    state = field[0, 0]
    source = source[0, 0]
    inverse = block_inverse[0, 0]
    coupling = coupling[0, 0]
    base = donor_base[0, 0]
    weight = donor_weight[0, 0]
    target = receiver_cell[0, 0]
    comps, rows, cols = state.shape
    faces = coupling.shape[0]
    blocks, slots = base.shape
    groups = lax.axis_size("group")
    swap = [(g * blocks + b, (groups - 1 - g) * blocks + b) for g in range(groups) for b in range(blocks)]
    up = [(b, b + 1) for b in range(blocks - 1)]
    down = [(b + 1, b) for b in range(blocks - 1)]

    def f32(*shape):
        return jax.ShapeDtypeStruct(shape, F32)

    def call(kernel, operands, remote, outs, scratch):
        remote = [pltpu.with_memory_space_constraint(value, pltpu.HBM) for value in remote]
        return pl.pallas_call(
            kernel,
            out_shape=outs,
            in_specs=vmem(len(operands)) + [pl.BlockSpec(memory_space=pltpu.HBM)] * len(remote),
            out_specs=tuple(vmem(len(outs))),
            scratch_shapes=scratch,
            compiler_params=pltpu.CompilerParams(vmem_limit_bytes=VMEM_LIMIT),
        )(*operands, *remote)

    def vmem_like(*shape, dtype=F32):
        return pltpu.VMEM(shape, dtype)

    fixed = comps * comps + comps + faces + 1
    cells = f32(comps, rows, cols)
    sums_shape = f32(blocks, -(-3 * comps // ROWS) * ROWS, slots)
    deep = blocks * slots // cols

    sums, top, bottom = call(
        start_kernel,
        (),
        (state, base, weight, target, source, inverse, coupling),
        (
            sums_shape,
            f32(comps * LOW + (fixed - 1) * LOW_DONE + deep, cols),
            f32(comps * HIGH + (fixed - 1) * HIGH_DONE + deep, cols),
        ),
        [
            vmem_like(comps, rows, cols),
            vmem_like(blocks, slots, dtype=jnp.int32),
            vmem_like(*weight.shape),
            vmem_like(blocks, slots, dtype=jnp.int32),
            vmem_like(2, comps, ROWS, cols),
            vmem_like(2, comps, comps, ROWS, cols),
            vmem_like(2, faces, ROWS, cols),
            pltpu.SemaphoreType.DMA((10,)),
        ],
    )

    placing = [vmem_like(comps * rows, cols), vmem_like(comps * (cols // LANES) * (ROWS // 2), 2 * LANES)]
    working = [vmem_like(comps, rows + 2 * PAD, cols)] * 2
    held = {"source": source, "inverse": inverse, "coupling": coupling, "base": base, "weight": weight}
    border = (f32(comps * LOW, cols), f32(comps * HIGH, cols))
    halo = f32(comps, ROWS, cols)
    for iteration in range(ITERS):
        arrived = lax.ppermute(sums, ("group", "blk"), swap)
        arrived = lax.all_to_all(arrived, "blk", split_axis=0, concat_axis=0, tiled=True)
        below = lax.ppermute(top, "blk", up)
        above = lax.ppermute(bottom, "blk", down)
        is_last = iteration == ITERS - 1
        if iteration == 0:
            cells_of = jax.ShapeDtypeStruct((blocks, slots), jnp.int32)
            (movable,) = call(
                frozen_kernel, (target,), (), (f32(rows, cols),), [vmem_like(rows, cols)]
            )
            held["low"], held["high"], low_target, high_target, below, above = call(
                partial(unpack_kernel, comps=comps, rows=rows),
                (below, above),
                (),
                (f32(fixed, ROWS, cols), f32(fixed, ROWS, cols), cells_of, cells_of, *border),
                [vmem_like((cols // LANES) * (ROWS // 2), 2 * LANES), vmem_like(1, ROWS, cols)],
            )
        names = tuple(held)
        near = tuple(pltpu.VMEM(held[name].shape, held[name].dtype) for name in names)
        state, placed_below, placed_above, *near = call(
            lambda *refs: place_kernel(len(names), refs),
            (arrived, target, state, movable, low_target, high_target),
            tuple(held[name] for name in names),
            (cells, halo, halo, *near),
            placing + [pltpu.SemaphoreType.DMA((len(names),))],
        )
        results = call(
            lambda *refs: step_kernel(names, is_last, refs),
            (state, below, above, placed_below, placed_above, movable, *near),
            (),
            (cells,) if is_last else (cells, sums_shape, *border),
            working,
        )
        state = results[0]
        if not is_last:
            sums, top, bottom = results[1:]
    return state[None, None]


def solution(mesh):
    in_specs = (
        P("group", "blk", None, None, None),
        P("group", "blk", None, None, None),
        P("group", "blk", None, None, None, None),
        P("group", "blk", None, None, None),
        P("group", "blk", None, None),
        P("group", "blk", None, None, None),
        P("group", "blk", None, None),
    )
    out_specs = P("group", "blk", None, None, None)
    return jax.shard_map(
        on_device, mesh=mesh, in_specs=in_specs, out_specs=out_specs, check_vma=False
    )
```

```python
from functools import partial

import jax
import jax.numpy as jnp
from jax import lax
from jax.experimental import pallas as pl
from jax.experimental.pallas import tpu as pltpu
from jax.sharding import PartitionSpec as P


ITERS = 4

upwind_offsets = (-3, -2, -1, 0, 1, 2)
upwind_weights = (-2.0 / 60.0, 15.0 / 60.0, -60.0 / 60.0, 20.0 / 60.0, 30.0 / 60.0, -3.0 / 60.0)

F32 = jnp.float32
BF16 = jnp.bfloat16
ROWS = 8
LOW, HIGH = 6, 4
LOW_DONE, HIGH_DONE = 3, 2
PAD = 2 * ROWS
LANES, LANE_BITS, GROUP_BITS = 128, 7, 2
UNROLL = 16
VMEM_LIMIT = 16 * 1024 * 1024


def vmem(count):
    return [pl.BlockSpec(memory_space=pltpu.VMEM)] * count


def divmod_const(value, size):
    if size & (size - 1) == 0:
        return value >> (size.bit_length() - 1), value & (size - 1)
    quotient = lax.div(value, jnp.int32(size))
    return quotient, value - quotient * size


def one_hot(index, size, packed=False):
    rows = lax.broadcasted_iota(jnp.int32, (size, index.shape[1]), 0)
    if size > 512 or not packed:
        return jnp.where(rows == index, 1.0, 0.0).astype(BF16)
    middle = size // 2
    rows = (rows - middle).astype(F32).astype(BF16)
    index = (index - middle).astype(F32).astype(BF16)
    return jnp.where(rows == index, jnp.array(1.0, BF16), jnp.array(0.0, BF16))


def split(value):
    high = value.astype(BF16)
    low = (value - high.astype(F32)).astype(BF16)
    return high, low


def repeat(count, step, unroll=UNROLL):
    lax.fori_loop(0, count, lambda i, carry: (step(i), carry)[1], 0, unroll=min(count, unroll))


def donor_sums(state, base_ref, weight_ref, out_ref):
    comps, rows, cols = state.shape
    half = cols // 2
    flat = state.reshape(comps * rows, cols)
    stacked = jnp.concatenate(split(flat), axis=0)
    at = lax.broadcasted_iota(jnp.int32, (cols, cols), 0)
    to = lax.broadcasted_iota(jnp.int32, (cols, cols), 1)
    source_col = jnp.where(to < half, 2 * to, 2 * (to - half) + 1)
    order = jnp.where(at == source_col, 1.0, 0.0).astype(BF16)
    ordered = jnp.dot(stacked, order, preferred_element_type=F32).astype(BF16)
    even, odd = ordered[:, :half], ordered[:, half:]
    blocks, slots = base_ref.shape
    row_iota = lax.broadcasted_iota(jnp.int32, (rows, slots), 0)

    def one(d):
        base = base_ref[pl.ds(d, 1), :]
        w0 = weight_ref[0, pl.ds(d, 1), :]
        w1 = weight_ref[1, pl.ds(d, 1), :]
        w2 = weight_ref[2, pl.ds(d, 1), :]
        w3 = weight_ref[3, pl.ds(d, 1), :]
        row, col = divmod_const(base, cols)
        is_odd = (col & 1) == 1
        wraps = col == cols - 1
        odd_at = col >> 1
        even_at = jnp.where(wraps, 0, (col + 1) >> 1)
        even_row = row + jnp.where(wraps, 1, 0)
        picked_even = jnp.dot(even, one_hot(even_at, half, True), preferred_element_type=F32)
        picked_odd = jnp.dot(odd, one_hot(odd_at, half, True), preferred_element_type=F32)
        count = comps * rows
        picked_even = (picked_even[:count] + picked_even[count:]).reshape(comps, rows, slots)
        picked_odd = (picked_odd[:count] + picked_odd[count:]).reshape(comps, rows, slots)
        even_weight = jnp.where(
            row_iota == even_row,
            jnp.where(is_odd, w1, w0),
            jnp.where(row_iota == even_row + 1, jnp.where(is_odd, w3, w2), 0.0),
        )
        odd_weight = jnp.where(
            row_iota == row,
            jnp.where(is_odd, w0, w1),
            jnp.where(row_iota == row + 1, jnp.where(is_odd, w2, w3), 0.0),
        )
        total = even_weight[None] * picked_even + odd_weight[None] * picked_odd
        out_ref[d, 0:comps, :] = jnp.sum(total, axis=1)

    repeat(blocks, one)
    none = jnp.zeros((comps, slots), F32)
    for d in range(blocks):
        out_ref[d, comps : 2 * comps, :] = out_ref[d - 1, 0:comps, :] if d > 0 else none
        out_ref[d, 2 * comps : 3 * comps, :] = out_ref[d + 1, 0:comps, :] if d < blocks - 1 else none


def selected(hit, values):
    count = values.shape[0] * hit.shape[0]
    parts = [
        jnp.where(hit[None], part.astype(F32)[:, None, :], 0.0).reshape(count, -1).astype(BF16)
        for part in split(values)
    ]
    return jnp.concatenate(parts, axis=0)


def add_product(acc_ref, left, right):
    out = lax.dot_general(left, right, (((1,), (1,)), ((), ())), preferred_element_type=F32)
    count = acc_ref.shape[0]
    acc_ref[...] += out if left.shape[0] == count else out[:count] + out[count:]


def frozen_kernel(target_ref, movable_ref, acc_ref):
    rows, cols = movable_ref.shape
    blocks, slots = target_ref.shape
    row_iota = lax.broadcasted_iota(jnp.int32, (rows, slots), 0)
    acc_ref[...] = jnp.zeros_like(acc_ref)

    def one(b):
        row, col = divmod_const(target_ref[pl.ds(b, 1), :], cols)
        add_product(acc_ref, jnp.where(row_iota == row, 1.0, 0.0).astype(BF16), one_hot(col, cols))

    repeat(blocks, one, 4)
    movable_ref[...] = jnp.where(acc_ref[...] > 0.5, 0.0, 1.0)


def place_own(arrived_ref, target_ref, comps, rows, cols, acc_ref):
    blocks, slots = target_ref.shape
    row_iota = lax.broadcasted_iota(jnp.int32, (rows, slots), 0)
    acc_ref[...] = jnp.zeros_like(acc_ref)

    def one(b):
        row, col = divmod_const(target_ref[pl.ds(b, 1), :], cols)
        left = selected(row_iota == row, arrived_ref[b, 0:comps, :])
        add_product(acc_ref, left, one_hot(col, cols))

    repeat(blocks, one)


def place_halo(arrived_ref, first, target_ref, start, comps, cols, acc_ref, out_ref, unroll=UNROLL):
    blocks, slots = target_ref.shape
    tiles = cols // LANES
    group = ROWS // 2
    row_iota = lax.broadcasted_iota(jnp.int32, (tiles * group, slots), 0)
    acc_ref[...] = jnp.zeros_like(acc_ref)

    def one(b):
        row, col = divmod_const(target_ref[pl.ds(b, 1), :], cols)
        row = row - start
        hit = row_iota == (col >> LANE_BITS) * group + (row & (group - 1))
        at = (row >> GROUP_BITS) * LANES + (col & (LANES - 1))
        if arrived_ref is None:
            left = jnp.where(hit, 1.0, 0.0).astype(BF16)
        else:
            left = selected(hit, arrived_ref[b, first : first + comps, :])
        add_product(acc_ref, left, one_hot(at, 2 * LANES))

    repeat(blocks, one, unroll)
    for c in range(comps):
        for t in range(tiles):
            for h in range(2):
                out_ref[c, h * group : (h + 1) * group, t * LANES : (t + 1) * LANES] = acc_ref[
                    (c * tiles + t) * group : (c * tiles + t + 1) * group,
                    h * LANES : (h + 1) * LANES,
                ]


def border_rows(state_ref, movable_ref, top_ref, bottom_ref):
    comps, rows, _ = state_ref.shape
    upper = movable_ref[rows - ROWS :, :] > 0.5
    lower = movable_ref[:ROWS, :] > 0.5
    for c in range(comps):
        kept = jnp.where(upper, state_ref[c, rows - ROWS :, :], 0.0)
        top_ref[c * LOW : (c + 1) * LOW, :] = kept[ROWS - LOW :, :]
        kept = jnp.where(lower, state_ref[c, :ROWS, :], 0.0)
        bottom_ref[c * HIGH : (c + 1) * HIGH, :] = kept[:HIGH, :]


def start_kernel(
    field_hbm, base_hbm, weight_hbm, target_hbm, source_hbm, inverse_hbm, coupling_hbm,
    sums_ref, top_ref, bottom_ref,
    field_ref, base_ref, weight_ref, target_ref, source_ref, inverse_ref, coupling_ref, sems,
):
    comps, rows, cols = field_ref.shape
    blocks, slots = target_ref.shape
    last = slice(rows - ROWS, rows)
    first = slice(0, ROWS)
    copies = [
        (field_hbm, field_ref),
        (base_hbm, base_ref),
        (weight_hbm, weight_ref),
        (target_hbm, target_ref),
        (source_hbm.at[:, last], source_ref.at[0]),
        (source_hbm.at[:, first], source_ref.at[1]),
        (inverse_hbm.at[:, :, last], inverse_ref.at[0]),
        (inverse_hbm.at[:, :, first], inverse_ref.at[1]),
        (coupling_hbm.at[:, last], coupling_ref.at[0]),
        (coupling_hbm.at[:, first], coupling_ref.at[1]),
    ]
    copies = [pltpu.make_async_copy(a, b, sems.at[i]) for i, (a, b) in enumerate(copies)]
    for copy in copies:
        copy.start()
    for copy in copies[:3]:
        copy.wait()
    donor_sums(field_ref[...], base_ref, weight_ref, sums_ref)
    for c in range(comps):
        top_ref[c * LOW : (c + 1) * LOW, :] = field_ref[c, rows - LOW :, :]
        bottom_ref[c * HIGH : (c + 1) * HIGH, :] = field_ref[c, :HIGH, :]
    for copy in copies[3:]:
        copy.wait()
    sides = (
        (top_ref, 0, comps * LOW, LOW_DONE, ROWS - LOW_DONE),
        (bottom_ref, 1, comps * HIGH, HIGH_DONE, 0),
    )
    for ref, side, offset, count, at in sides:
        fixed = [inverse_ref[side, v, w] for v in range(comps) for w in range(comps)]
        fixed += [source_ref[side, w] for w in range(comps)]
        fixed += [coupling_ref[side, i] for i in range(coupling_ref.shape[1])]
        for value in fixed:
            ref[offset : offset + count, :] = value[at : at + count, :]
            offset += count
        per = cols // slots
        deep = blocks // per
        for i in range(per):
            cells = target_ref[i * deep : (i + 1) * deep, :].astype(F32)
            ref[offset : offset + deep, i * slots : (i + 1) * slots] = cells


def unpack_kernel(
    top_ref, bottom_ref, low_ref, high_ref, low_target_ref, high_target_ref, below_ref, above_ref,
    acc_ref, count_ref, *, comps, rows,
):
    cols = top_ref.shape[1]
    sublanes = lax.broadcasted_iota(jnp.int32, (ROWS, cols), 0)
    sides = (
        (top_ref, LOW, LOW_DONE, ROWS - LOW, ROWS - LOW_DONE, rows - ROWS, low_ref, low_target_ref, below_ref),
        (bottom_ref, HIGH, HIGH_DONE, 0, 0, 0, high_ref, high_target_ref, above_ref),
    )
    for ref, wide, count, wide_at, at, start, out_ref, target_ref, halo_ref in sides:
        blocks, slots = target_ref.shape
        offset = comps * wide
        last = out_ref.shape[0] - 1
        for i in range(last):
            out_ref[i] = jnp.zeros((ROWS, cols), F32)
            out_ref[i, at : at + count, :] = ref[offset : offset + count, :]
            offset += count
        per = cols // slots
        deep = blocks // per
        for i in range(per):
            cells = ref[offset : offset + deep, i * slots : (i + 1) * slots]
            target_ref[i * deep : (i + 1) * deep, :] = cells.astype(jnp.int32)
        place_halo(None, 0, target_ref, start, 1, cols, acc_ref, count_ref, 4)
        movable = count_ref[0] < 0.5
        done = (sublanes >= at) & (sublanes < at + count)
        out_ref[last] = jnp.where(movable & done, 1.0, 0.0)
        movable = count_ref[0, wide_at : wide_at + wide, :] < 0.5
        for c in range(comps):
            halo_ref[c * wide : (c + 1) * wide, :] = jnp.where(
                movable, ref[c * wide : (c + 1) * wide, :], 0.0
            )


def place(
    arrived_ref, target_ref, state_ref, movable_ref, low_target_ref, high_target_ref,
    out_ref, below_ref, above_ref, acc_ref, halo_ref,
):
    comps, rows, cols = state_ref.shape
    place_own(arrived_ref, target_ref, comps, rows, cols, acc_ref)
    movable = movable_ref[...] > 0.5
    for c in range(comps):
        out_ref[c] = jnp.where(movable, state_ref[c], acc_ref[c * rows : (c + 1) * rows, :])
    place_halo(arrived_ref, comps, low_target_ref, rows - ROWS, comps, cols, halo_ref, below_ref)
    place_halo(arrived_ref, 2 * comps, high_target_ref, 0, comps, cols, halo_ref, above_ref)


def load(ref, c, start, count):
    return jnp.concatenate(
        [ref[c, t, start : start + count, :] for t in range(ref.shape[1])], axis=1
    )


def store(ref, c, start, value):
    for t in range(ref.shape[1]):
        ref[c, t, start : start + value.shape[0], :] = value[:, t * LANES : (t + 1) * LANES]


def sections(u_ref, start, parts, write, is_near, parity, comps, cols):
    source, inverse, coupling, movable = parts
    lanes = lax.broadcasted_iota(jnp.int32, (ROWS, cols), 1)
    sublanes = lax.broadcasted_iota(jnp.int32, (ROWS, cols), 0)

    def rows_at(c, offset):
        return load(u_ref, c, start + offset, ROWS)

    def shifted(value, offset):
        return pltpu.roll(value, (-offset) % cols, 1)

    def finish(update, terms, mask):
        for v in range(comps):
            total = update(v)
            for w in range(comps):
                product = inverse(v, w) * terms[w]
                total = product if total is None else total + product
            write(v, jnp.where(mask, total, rows_at(v, 0)))

    @pl.when(is_near)
    def _():
        c0, c1, c2, c3 = (coupling(i) for i in range(4))
        c2 = jnp.where(lanes >= 1, c2, 0.0)
        c3 = jnp.where(lanes < cols - 1, c3, 0.0)
        terms = []
        for w in range(comps):
            here = rows_at(w, 0)
            term = source(w) + c0 * rows_at(w, -1) + c1 * rows_at(w, 1)
            terms.append(term + c2 * shifted(here, -1) + c3 * shifted(here, 1))
        colour = ((lanes + sublanes) & 1) == parity
        finish(lambda v: None, terms, colour & (movable() > 0.5))

    @pl.when(jnp.logical_not(is_near))
    def _():
        c0, c1 = coupling(0), coupling(1)
        factors = []
        for offset, weight in zip(upwind_offsets, upwind_weights):
            inside = (lanes + offset >= 0) & (lanes + offset < cols)
            factors.append(weight if offset == 0 else jnp.where(inside, weight, 0.0))
        terms = []
        for w in range(comps):
            here = rows_at(w, 0)
            along_j = along_k = None
            for offset, weight, factor in zip(upwind_offsets, upwind_weights, factors):
                in_j = weight * rows_at(w, offset)
                in_k = factor * (here if offset == 0 else shifted(here, offset))
                along_j = in_j if along_j is None else along_j + in_j
                along_k = in_k if along_k is None else along_k + in_k
            terms.append(source(w) - c0 * along_j - c1 * along_k)
        finish(lambda v: rows_at(v, 0), terms, movable() > 0.5)


def sweep(state_ref, below_ref, above_ref, placed_below_ref, placed_above_ref, movable_ref, work, out_ref):
    comps, rows, cols = state_ref.shape
    source_ref, inverse_ref, coupling_ref = work["source"], work["inverse"], work["coupling"]
    low_ref, high_ref, u_ref, v_ref = work["low"], work["high"], work["u"], work["v"]
    is_near = lax.axis_index("group") == 0
    for c in range(comps):
        store(u_ref, c, PAD, state_ref[c])
        below = below_ref[c * LOW : (c + 1) * LOW, :] + placed_below_ref[c, ROWS - LOW :, :]
        store(u_ref, c, PAD - LOW, below)
        above = above_ref[c * HIGH : (c + 1) * HIGH, :] + placed_above_ref[c, :HIGH, :]
        store(u_ref, c, PAD + rows, above)

    def own(r):
        at = slice(r, r + ROWS)
        return (
            lambda w: source_ref[w, at, :],
            lambda v, w: inverse_ref[v, w, at, :],
            lambda i: coupling_ref[i, at, :],
            lambda: movable_ref[at, :],
        )

    def packed(ref):
        first = comps * comps
        second = first + comps
        last = ref.shape[0] - 1
        return (
            lambda w: ref[first + w],
            lambda v, w: ref[v * comps + w],
            lambda i: ref[second + i],
            lambda: ref[last],
        )

    def into(start):
        return lambda v, value: store(v_ref, v, start, value)

    def out_of(start):
        def write(v, value):
            out_ref[v, start : start + ROWS, :] = value

        return write

    for r in range(0, rows, ROWS):
        sections(u_ref, PAD + r, own(r), into(PAD + r), is_near, 0, comps, cols)
    sections(u_ref, PAD - ROWS, packed(low_ref), into(PAD - ROWS), is_near, 0, comps, cols)
    sections(u_ref, PAD + rows, packed(high_ref), into(PAD + rows), is_near, 0, comps, cols)
    for r in range(0, rows, ROWS):
        sections(v_ref, PAD + r, own(r), out_of(r), is_near, 1, comps, cols)


def place_kernel(count, refs):
    refs = list(refs)
    operands, refs = refs[:6], refs[6:]
    held, refs = refs[:count], refs[count:]
    results, refs = refs[:3], refs[3:]
    copied, (acc_ref, halo_ref, sems) = refs[:count], refs[count:]
    copies = [pltpu.make_async_copy(held[i], copied[i], sems.at[i]) for i in range(count)]
    for copy in copies:
        copy.start()
    place(*operands, *results, acc_ref, halo_ref)
    for copy in copies:
        copy.wait()


def step_kernel(names, is_last, refs):
    refs = list(refs)
    operands, refs = refs[:6], refs[6:]
    work, refs = dict(zip(names, refs)), refs[len(names) :]
    out_ref = refs.pop(0)
    if not is_last:
        sums_ref, top_ref, bottom_ref = refs[:3]
        refs = refs[3:]
    work["u"], work["v"] = refs
    sweep(*operands, work, out_ref)
    if not is_last:
        border_rows(out_ref, operands[5], top_ref, bottom_ref)
        donor_sums(out_ref[...], work["base"], work["weight"], sums_ref)


def on_device(field, source, block_inverse, coupling, donor_base, donor_weight, receiver_cell):
    state = field[0, 0]
    source = source[0, 0]
    inverse = block_inverse[0, 0]
    coupling = coupling[0, 0]
    base = donor_base[0, 0]
    weight = donor_weight[0, 0]
    target = receiver_cell[0, 0]
    comps, rows, cols = state.shape
    faces = coupling.shape[0]
    blocks, slots = base.shape
    groups = lax.axis_size("group")
    swap = [(g * blocks + b, (groups - 1 - g) * blocks + b) for g in range(groups) for b in range(blocks)]
    up = [(b, b + 1) for b in range(blocks - 1)]
    down = [(b + 1, b) for b in range(blocks - 1)]

    def f32(*shape):
        return jax.ShapeDtypeStruct(shape, F32)

    def call(kernel, operands, remote, outs, scratch):
        remote = [pltpu.with_memory_space_constraint(value, pltpu.HBM) for value in remote]
        return pl.pallas_call(
            kernel,
            out_shape=outs,
            in_specs=vmem(len(operands)) + [pl.BlockSpec(memory_space=pltpu.HBM)] * len(remote),
            out_specs=tuple(vmem(len(outs))),
            scratch_shapes=scratch,
            compiler_params=pltpu.CompilerParams(vmem_limit_bytes=VMEM_LIMIT),
        )(*operands, *remote)

    def vmem_like(*shape, dtype=F32):
        return pltpu.VMEM(shape, dtype)

    fixed = comps * comps + comps + faces + 1
    cells = f32(comps, rows, cols)
    sums_shape = f32(blocks, -(-3 * comps // ROWS) * ROWS, slots)
    deep = blocks * slots // cols

    sums, top, bottom = call(
        start_kernel,
        (),
        (state, base, weight, target, source, inverse, coupling),
        (
            sums_shape,
            f32(comps * LOW + (fixed - 1) * LOW_DONE + deep, cols),
            f32(comps * HIGH + (fixed - 1) * HIGH_DONE + deep, cols),
        ),
        [
            vmem_like(comps, rows, cols),
            vmem_like(blocks, slots, dtype=jnp.int32),
            vmem_like(*weight.shape),
            vmem_like(blocks, slots, dtype=jnp.int32),
            vmem_like(2, comps, ROWS, cols),
            vmem_like(2, comps, comps, ROWS, cols),
            vmem_like(2, faces, ROWS, cols),
            pltpu.SemaphoreType.DMA((10,)),
        ],
    )

    placing = [vmem_like(comps * rows, cols), vmem_like(comps * (cols // LANES) * (ROWS // 2), 2 * LANES)]
    working = [vmem_like(comps, cols // LANES, rows + 2 * PAD, LANES)] * 2
    held = {"source": source, "inverse": inverse, "coupling": coupling, "base": base, "weight": weight}
    border = (f32(comps * LOW, cols), f32(comps * HIGH, cols))
    halo = f32(comps, ROWS, cols)
    for iteration in range(ITERS):
        arrived = lax.ppermute(sums, ("group", "blk"), swap)
        arrived = lax.all_to_all(arrived, "blk", split_axis=0, concat_axis=0, tiled=True)
        below = lax.ppermute(top, "blk", up)
        above = lax.ppermute(bottom, "blk", down)
        is_last = iteration == ITERS - 1
        if iteration == 0:
            cells_of = jax.ShapeDtypeStruct((blocks, slots), jnp.int32)
            (movable,) = call(
                frozen_kernel, (target,), (), (f32(rows, cols),), [vmem_like(rows, cols)]
            )
            held["low"], held["high"], low_target, high_target, below, above = call(
                partial(unpack_kernel, comps=comps, rows=rows),
                (below, above),
                (),
                (f32(fixed, ROWS, cols), f32(fixed, ROWS, cols), cells_of, cells_of, *border),
                [vmem_like((cols // LANES) * (ROWS // 2), 2 * LANES), vmem_like(1, ROWS, cols)],
            )
        names = tuple(held)
        near = tuple(pltpu.VMEM(held[name].shape, held[name].dtype) for name in names)
        state, placed_below, placed_above, *near = call(
            lambda *refs: place_kernel(len(names), refs),
            (arrived, target, state, movable, low_target, high_target),
            tuple(held[name] for name in names),
            (cells, halo, halo, *near),
            placing + [pltpu.SemaphoreType.DMA((len(names),))],
        )
        results = call(
            lambda *refs: step_kernel(names, is_last, refs),
            (state, below, above, placed_below, placed_above, movable, *near),
            (),
            (cells,) if is_last else (cells, sums_shape, *border),
            working,
        )
        state = results[0]
        if not is_last:
            sums, top, bottom = results[1:]
    return state[None, None]


def solution(mesh):
    in_specs = (
        P("group", "blk", None, None, None),
        P("group", "blk", None, None, None),
        P("group", "blk", None, None, None, None),
        P("group", "blk", None, None, None),
        P("group", "blk", None, None),
        P("group", "blk", None, None, None),
        P("group", "blk", None, None),
    )
    out_specs = P("group", "blk", None, None, None)
    return jax.shard_map(
        on_device, mesh=mesh, in_specs=in_specs, out_specs=out_specs, check_vma=False
    )
```

```python
from functools import partial

import jax
import jax.numpy as jnp
from jax import lax
from jax.experimental import pallas as pl
from jax.experimental.pallas import tpu as pltpu
from jax.sharding import PartitionSpec as P


ITERS = 4

upwind_offsets = (-3, -2, -1, 0, 1, 2)
upwind_weights = (-2.0 / 60.0, 15.0 / 60.0, -60.0 / 60.0, 20.0 / 60.0, 30.0 / 60.0, -3.0 / 60.0)

F32 = jnp.float32
BF16 = jnp.bfloat16
ROWS = 8
LOW, HIGH = 6, 4
LOW_DONE, HIGH_DONE = 3, 2
PAD = 2 * ROWS
LANES, LANE_BITS, GROUP_BITS = 128, 7, 2
UNROLL = 16
VMEM_LIMIT = 16 * 1024 * 1024


def vmem(count):
    return [pl.BlockSpec(memory_space=pltpu.VMEM)] * count


def divmod_const(value, size):
    if size & (size - 1) == 0:
        return value >> (size.bit_length() - 1), value & (size - 1)
    quotient = lax.div(value, jnp.int32(size))
    return quotient, value - quotient * size


def one_hot(index, size, packed=False):
    rows = lax.broadcasted_iota(jnp.int32, (size, index.shape[1]), 0)
    if size > 512 or not packed:
        return jnp.where(rows == index, 1.0, 0.0).astype(BF16)
    middle = size // 2
    rows = (rows - middle).astype(F32).astype(BF16)
    index = (index - middle).astype(F32).astype(BF16)
    return jnp.where(rows == index, jnp.array(1.0, BF16), jnp.array(0.0, BF16))


def split(value):
    high = value.astype(BF16)
    low = (value - high.astype(F32)).astype(BF16)
    return high, low


def repeat(count, step, unroll=UNROLL):
    lax.fori_loop(0, count, lambda i, carry: (step(i), carry)[1], 0, unroll=min(count, unroll))


def donor_sums(state, base_ref, weight_ref, out_ref):
    comps, rows, cols = state.shape
    half = cols // 2
    flat = state.reshape(comps * rows, cols)
    stacked = jnp.concatenate(split(flat), axis=0)
    at = lax.broadcasted_iota(jnp.int32, (cols, cols), 0)
    to = lax.broadcasted_iota(jnp.int32, (cols, cols), 1)
    source_col = jnp.where(to < half, 2 * to, 2 * (to - half) + 1)
    order = jnp.where(at == source_col, 1.0, 0.0).astype(BF16)
    ordered = jnp.dot(stacked, order, preferred_element_type=F32).astype(BF16)
    even, odd = ordered[:, :half], ordered[:, half:]
    blocks, slots = base_ref.shape
    row_iota = lax.broadcasted_iota(jnp.int32, (rows, slots), 0)

    def one(d):
        base = base_ref[pl.ds(d, 1), :]
        w0 = weight_ref[0, pl.ds(d, 1), :]
        w1 = weight_ref[1, pl.ds(d, 1), :]
        w2 = weight_ref[2, pl.ds(d, 1), :]
        w3 = weight_ref[3, pl.ds(d, 1), :]
        row, col = divmod_const(base, cols)
        is_odd = (col & 1) == 1
        wraps = col == cols - 1
        odd_at = col >> 1
        even_at = jnp.where(wraps, 0, (col + 1) >> 1)
        even_row = row + jnp.where(wraps, 1, 0)
        picked_even = jnp.dot(even, one_hot(even_at, half, True), preferred_element_type=F32)
        picked_odd = jnp.dot(odd, one_hot(odd_at, half, True), preferred_element_type=F32)
        count = comps * rows
        picked_even = (picked_even[:count] + picked_even[count:]).reshape(comps, rows, slots)
        picked_odd = (picked_odd[:count] + picked_odd[count:]).reshape(comps, rows, slots)
        even_weight = jnp.where(
            row_iota == even_row,
            jnp.where(is_odd, w1, w0),
            jnp.where(row_iota == even_row + 1, jnp.where(is_odd, w3, w2), 0.0),
        )
        odd_weight = jnp.where(
            row_iota == row,
            jnp.where(is_odd, w0, w1),
            jnp.where(row_iota == row + 1, jnp.where(is_odd, w2, w3), 0.0),
        )
        total = even_weight[None] * picked_even + odd_weight[None] * picked_odd
        values = jnp.sum(total, axis=1)
        out_ref[d, 0:comps, :] = values
        return values

    none = jnp.zeros((comps, slots), F32)
    if blocks <= UNROLL:
        out_ref[0, comps : 2 * comps, :] = none
        out_ref[blocks - 1, 2 * comps : 3 * comps, :] = none
        for d in range(blocks):
            values = one(d)
            if d < blocks - 1:
                out_ref[d + 1, comps : 2 * comps, :] = values
            if d > 0:
                out_ref[d - 1, 2 * comps : 3 * comps, :] = values
        return
    repeat(blocks, one)
    for d in range(blocks):
        out_ref[d, comps : 2 * comps, :] = out_ref[d - 1, 0:comps, :] if d > 0 else none
        out_ref[d, 2 * comps : 3 * comps, :] = out_ref[d + 1, 0:comps, :] if d < blocks - 1 else none


def selected(hit, values):
    count = values.shape[0] * hit.shape[0]
    parts = [
        jnp.where(hit[None], part.astype(F32)[:, None, :], 0.0).reshape(count, -1).astype(BF16)
        for part in split(values)
    ]
    return jnp.concatenate(parts, axis=0)


def add_product(acc_ref, left, right):
    out = lax.dot_general(left, right, (((1,), (1,)), ((), ())), preferred_element_type=F32)
    count = acc_ref.shape[0]
    acc_ref[...] += out if left.shape[0] == count else out[:count] + out[count:]


def frozen_kernel(target_ref, movable_ref, acc_ref):
    rows, cols = movable_ref.shape
    blocks, slots = target_ref.shape
    row_iota = lax.broadcasted_iota(jnp.int32, (rows, slots), 0)
    acc_ref[...] = jnp.zeros_like(acc_ref)

    def one(b):
        row, col = divmod_const(target_ref[pl.ds(b, 1), :], cols)
        add_product(acc_ref, jnp.where(row_iota == row, 1.0, 0.0).astype(BF16), one_hot(col, cols))

    repeat(blocks, one, 4)
    movable_ref[...] = jnp.where(acc_ref[...] > 0.5, 0.0, 1.0)


def place_own(arrived_ref, target_ref, comps, rows, cols, acc_ref):
    blocks, slots = target_ref.shape
    row_iota = lax.broadcasted_iota(jnp.int32, (rows, slots), 0)
    acc_ref[...] = jnp.zeros_like(acc_ref)

    def one(b):
        row, col = divmod_const(target_ref[pl.ds(b, 1), :], cols)
        left = selected(row_iota == row, arrived_ref[b, 0:comps, :])
        add_product(acc_ref, left, one_hot(col, cols))

    repeat(blocks, one)


def place_halo(arrived_ref, first, target_ref, start, comps, cols, acc_ref, out_ref, unroll=UNROLL):
    blocks, slots = target_ref.shape
    tiles = cols // LANES
    group = ROWS // 2
    row_iota = lax.broadcasted_iota(jnp.int32, (tiles * group, slots), 0)
    acc_ref[...] = jnp.zeros_like(acc_ref)

    def one(b):
        row, col = divmod_const(target_ref[pl.ds(b, 1), :], cols)
        row = row - start
        hit = row_iota == (col >> LANE_BITS) * group + (row & (group - 1))
        at = (row >> GROUP_BITS) * LANES + (col & (LANES - 1))
        if arrived_ref is None:
            left = jnp.where(hit, 1.0, 0.0).astype(BF16)
        else:
            left = selected(hit, arrived_ref[b, first : first + comps, :])
        add_product(acc_ref, left, one_hot(at, 2 * LANES))

    repeat(blocks, one, unroll)
    for c in range(comps):
        for t in range(tiles):
            for h in range(2):
                out_ref[c, h * group : (h + 1) * group, t * LANES : (t + 1) * LANES] = acc_ref[
                    (c * tiles + t) * group : (c * tiles + t + 1) * group,
                    h * LANES : (h + 1) * LANES,
                ]


def border_rows(state_ref, movable_ref, top_ref, bottom_ref):
    comps, rows, _ = state_ref.shape
    upper = movable_ref[rows - ROWS :, :] > 0.5
    lower = movable_ref[:ROWS, :] > 0.5
    for c in range(comps):
        kept = jnp.where(upper, state_ref[c, rows - ROWS :, :], 0.0)
        top_ref[c * LOW : (c + 1) * LOW, :] = kept[ROWS - LOW :, :]
        kept = jnp.where(lower, state_ref[c, :ROWS, :], 0.0)
        bottom_ref[c * HIGH : (c + 1) * HIGH, :] = kept[:HIGH, :]


def start_kernel(
    field_hbm, base_hbm, weight_hbm, target_hbm, source_hbm, inverse_hbm, coupling_hbm,
    sums_ref, top_ref, bottom_ref,
    field_ref, base_ref, weight_ref, target_ref, source_ref, inverse_ref, coupling_ref, sems,
):
    comps, rows, cols = field_ref.shape
    blocks, slots = target_ref.shape
    last = slice(rows - ROWS, rows)
    first = slice(0, ROWS)
    copies = [
        (field_hbm, field_ref),
        (base_hbm, base_ref),
        (weight_hbm, weight_ref),
        (target_hbm, target_ref),
        (source_hbm.at[:, last], source_ref.at[0]),
        (source_hbm.at[:, first], source_ref.at[1]),
        (inverse_hbm.at[:, :, last], inverse_ref.at[0]),
        (inverse_hbm.at[:, :, first], inverse_ref.at[1]),
        (coupling_hbm.at[:, last], coupling_ref.at[0]),
        (coupling_hbm.at[:, first], coupling_ref.at[1]),
    ]
    copies = [pltpu.make_async_copy(a, b, sems.at[i]) for i, (a, b) in enumerate(copies)]
    for copy in copies:
        copy.start()
    for copy in copies[:3]:
        copy.wait()
    donor_sums(field_ref[...], base_ref, weight_ref, sums_ref)
    for c in range(comps):
        top_ref[c * LOW : (c + 1) * LOW, :] = field_ref[c, rows - LOW :, :]
        bottom_ref[c * HIGH : (c + 1) * HIGH, :] = field_ref[c, :HIGH, :]
    for copy in copies[3:]:
        copy.wait()
    sides = (
        (top_ref, 0, comps * LOW, LOW_DONE, ROWS - LOW_DONE),
        (bottom_ref, 1, comps * HIGH, HIGH_DONE, 0),
    )
    for ref, side, offset, count, at in sides:
        fixed = [inverse_ref[side, v, w] for v in range(comps) for w in range(comps)]
        fixed += [source_ref[side, w] for w in range(comps)]
        fixed += [coupling_ref[side, i] for i in range(coupling_ref.shape[1])]
        for value in fixed:
            ref[offset : offset + count, :] = value[at : at + count, :]
            offset += count
        per = cols // slots
        deep = blocks // per
        for i in range(per):
            cells = target_ref[i * deep : (i + 1) * deep, :].astype(F32)
            ref[offset : offset + deep, i * slots : (i + 1) * slots] = cells


def unpack_kernel(
    top_ref, bottom_ref, low_ref, high_ref, low_target_ref, high_target_ref, below_ref, above_ref,
    acc_ref, count_ref, *, comps, rows,
):
    cols = top_ref.shape[1]
    sublanes = lax.broadcasted_iota(jnp.int32, (ROWS, cols), 0)
    sides = (
        (top_ref, LOW, LOW_DONE, ROWS - LOW, ROWS - LOW_DONE, rows - ROWS, low_ref, low_target_ref, below_ref),
        (bottom_ref, HIGH, HIGH_DONE, 0, 0, 0, high_ref, high_target_ref, above_ref),
    )
    for ref, wide, count, wide_at, at, start, out_ref, target_ref, halo_ref in sides:
        blocks, slots = target_ref.shape
        offset = comps * wide
        last = out_ref.shape[0] - 1
        for i in range(last):
            out_ref[i] = jnp.zeros((ROWS, cols), F32)
            out_ref[i, at : at + count, :] = ref[offset : offset + count, :]
            offset += count
        per = cols // slots
        deep = blocks // per
        for i in range(per):
            cells = ref[offset : offset + deep, i * slots : (i + 1) * slots]
            target_ref[i * deep : (i + 1) * deep, :] = cells.astype(jnp.int32)
        place_halo(None, 0, target_ref, start, 1, cols, acc_ref, count_ref, 4)
        movable = count_ref[0] < 0.5
        done = (sublanes >= at) & (sublanes < at + count)
        out_ref[last] = jnp.where(movable & done, 1.0, 0.0)
        movable = count_ref[0, wide_at : wide_at + wide, :] < 0.5
        for c in range(comps):
            halo_ref[c * wide : (c + 1) * wide, :] = jnp.where(
                movable, ref[c * wide : (c + 1) * wide, :], 0.0
            )


def place(
    arrived_ref, target_ref, state_ref, movable_ref, low_target_ref, high_target_ref,
    out_ref, below_ref, above_ref, acc_ref, halo_ref,
):
    comps, rows, cols = state_ref.shape
    place_own(arrived_ref, target_ref, comps, rows, cols, acc_ref)
    movable = movable_ref[...] > 0.5
    for c in range(comps):
        out_ref[c] = jnp.where(movable, state_ref[c], acc_ref[c * rows : (c + 1) * rows, :])
    place_halo(arrived_ref, comps, low_target_ref, rows - ROWS, comps, cols, halo_ref, below_ref)
    place_halo(arrived_ref, 2 * comps, high_target_ref, 0, comps, cols, halo_ref, above_ref)


def load(ref, c, start, count):
    return jnp.concatenate(
        [ref[c, t, start : start + count, :] for t in range(ref.shape[1])], axis=1
    )


def store(ref, c, start, value):
    for t in range(ref.shape[1]):
        ref[c, t, start : start + value.shape[0], :] = value[:, t * LANES : (t + 1) * LANES]


def sections(u_ref, start, parts, write, is_near, parity, comps, cols):
    source, inverse, coupling, movable = parts
    lanes = lax.broadcasted_iota(jnp.int32, (ROWS, cols), 1)
    sublanes = lax.broadcasted_iota(jnp.int32, (ROWS, cols), 0)

    def rows_at(c, offset):
        return load(u_ref, c, start + offset, ROWS)

    def shifted(value, offset):
        return pltpu.roll(value, (-offset) % cols, 1)

    def finish(update, terms, mask):
        for v in range(comps):
            total = update(v)
            for w in range(comps):
                product = inverse(v, w) * terms[w]
                total = product if total is None else total + product
            write(v, jnp.where(mask, total, rows_at(v, 0)))

    @pl.when(is_near)
    def _():
        c0, c1, c2, c3 = (coupling(i) for i in range(4))
        c2 = jnp.where(lanes >= 1, c2, 0.0)
        c3 = jnp.where(lanes < cols - 1, c3, 0.0)
        terms = []
        for w in range(comps):
            here = rows_at(w, 0)
            term = source(w) + c0 * rows_at(w, -1) + c1 * rows_at(w, 1)
            terms.append(term + c2 * shifted(here, -1) + c3 * shifted(here, 1))
        colour = ((lanes + sublanes) & 1) == parity
        finish(lambda v: None, terms, colour & (movable() > 0.5))

    @pl.when(jnp.logical_not(is_near))
    def _():
        c0, c1 = coupling(0), coupling(1)
        factors = []
        for offset, weight in zip(upwind_offsets, upwind_weights):
            inside = (lanes + offset >= 0) & (lanes + offset < cols)
            factors.append(weight if offset == 0 else jnp.where(inside, weight, 0.0))
        terms = []
        for w in range(comps):
            here = rows_at(w, 0)
            along_j = along_k = None
            for offset, weight, factor in zip(upwind_offsets, upwind_weights, factors):
                in_j = weight * rows_at(w, offset)
                in_k = factor * (here if offset == 0 else shifted(here, offset))
                along_j = in_j if along_j is None else along_j + in_j
                along_k = in_k if along_k is None else along_k + in_k
            terms.append(source(w) - c0 * along_j - c1 * along_k)
        finish(lambda v: rows_at(v, 0), terms, movable() > 0.5)


def sweep(state_ref, below_ref, above_ref, placed_below_ref, placed_above_ref, movable_ref, work, out_ref):
    comps, rows, cols = state_ref.shape
    source_ref, inverse_ref, coupling_ref = work["source"], work["inverse"], work["coupling"]
    low_ref, high_ref, u_ref, v_ref = work["low"], work["high"], work["u"], work["v"]
    is_near = lax.axis_index("group") == 0
    for c in range(comps):
        store(u_ref, c, PAD, state_ref[c])
        below = below_ref[c * LOW : (c + 1) * LOW, :] + placed_below_ref[c, ROWS - LOW :, :]
        store(u_ref, c, PAD - LOW, below)
        above = above_ref[c * HIGH : (c + 1) * HIGH, :] + placed_above_ref[c, :HIGH, :]
        store(u_ref, c, PAD + rows, above)

    def own(r):
        at = slice(r, r + ROWS)
        return (
            lambda w: source_ref[w, at, :],
            lambda v, w: inverse_ref[v, w, at, :],
            lambda i: coupling_ref[i, at, :],
            lambda: movable_ref[at, :],
        )

    def packed(ref):
        first = comps * comps
        second = first + comps
        last = ref.shape[0] - 1
        return (
            lambda w: ref[first + w],
            lambda v, w: ref[v * comps + w],
            lambda i: ref[second + i],
            lambda: ref[last],
        )

    def into(start):
        return lambda v, value: store(v_ref, v, start, value)

    def out_of(start):
        def write(v, value):
            out_ref[v, start : start + ROWS, :] = value

        return write

    for r in range(0, rows, ROWS):
        sections(u_ref, PAD + r, own(r), into(PAD + r), is_near, 0, comps, cols)
    sections(u_ref, PAD - ROWS, packed(low_ref), into(PAD - ROWS), is_near, 0, comps, cols)
    sections(u_ref, PAD + rows, packed(high_ref), into(PAD + rows), is_near, 0, comps, cols)
    for r in range(0, rows, ROWS):
        sections(v_ref, PAD + r, own(r), out_of(r), is_near, 1, comps, cols)


def place_kernel(count, refs):
    refs = list(refs)
    operands, refs = refs[:6], refs[6:]
    held, refs = refs[:count], refs[count:]
    results, refs = refs[:3], refs[3:]
    copied, (acc_ref, halo_ref, sems) = refs[:count], refs[count:]
    copies = [pltpu.make_async_copy(held[i], copied[i], sems.at[i]) for i in range(count)]
    for copy in copies:
        copy.start()
    place(*operands, *results, acc_ref, halo_ref)
    for copy in copies:
        copy.wait()


def step_kernel(names, is_last, refs):
    refs = list(refs)
    operands, refs = refs[:6], refs[6:]
    work, refs = dict(zip(names, refs)), refs[len(names) :]
    out_ref = refs.pop(0)
    if not is_last:
        sums_ref, top_ref, bottom_ref = refs[:3]
        refs = refs[3:]
    work["u"], work["v"] = refs
    sweep(*operands, work, out_ref)
    if not is_last:
        border_rows(out_ref, operands[5], top_ref, bottom_ref)
        donor_sums(out_ref[...], work["base"], work["weight"], sums_ref)


def on_device(field, source, block_inverse, coupling, donor_base, donor_weight, receiver_cell):
    state = field[0, 0]
    source = source[0, 0]
    inverse = block_inverse[0, 0]
    coupling = coupling[0, 0]
    base = donor_base[0, 0]
    weight = donor_weight[0, 0]
    target = receiver_cell[0, 0]
    comps, rows, cols = state.shape
    faces = coupling.shape[0]
    blocks, slots = base.shape
    groups = lax.axis_size("group")
    swap = [(g * blocks + b, (groups - 1 - g) * blocks + b) for g in range(groups) for b in range(blocks)]
    up = [(b, b + 1) for b in range(blocks - 1)]
    down = [(b + 1, b) for b in range(blocks - 1)]

    def f32(*shape):
        return jax.ShapeDtypeStruct(shape, F32)

    def call(kernel, operands, remote, outs, scratch):
        remote = [pltpu.with_memory_space_constraint(value, pltpu.HBM) for value in remote]
        return pl.pallas_call(
            kernel,
            out_shape=outs,
            in_specs=vmem(len(operands)) + [pl.BlockSpec(memory_space=pltpu.HBM)] * len(remote),
            out_specs=tuple(vmem(len(outs))),
            scratch_shapes=scratch,
            compiler_params=pltpu.CompilerParams(vmem_limit_bytes=VMEM_LIMIT),
        )(*operands, *remote)

    def vmem_like(*shape, dtype=F32):
        return pltpu.VMEM(shape, dtype)

    fixed = comps * comps + comps + faces + 1
    cells = f32(comps, rows, cols)
    sums_shape = f32(blocks, -(-3 * comps // ROWS) * ROWS, slots)
    deep = blocks * slots // cols

    sums, top, bottom = call(
        start_kernel,
        (),
        (state, base, weight, target, source, inverse, coupling),
        (
            sums_shape,
            f32(comps * LOW + (fixed - 1) * LOW_DONE + deep, cols),
            f32(comps * HIGH + (fixed - 1) * HIGH_DONE + deep, cols),
        ),
        [
            vmem_like(comps, rows, cols),
            vmem_like(blocks, slots, dtype=jnp.int32),
            vmem_like(*weight.shape),
            vmem_like(blocks, slots, dtype=jnp.int32),
            vmem_like(2, comps, ROWS, cols),
            vmem_like(2, comps, comps, ROWS, cols),
            vmem_like(2, faces, ROWS, cols),
            pltpu.SemaphoreType.DMA((10,)),
        ],
    )

    placing = [vmem_like(comps * rows, cols), vmem_like(comps * (cols // LANES) * (ROWS // 2), 2 * LANES)]
    working = [vmem_like(comps, cols // LANES, rows + 2 * PAD, LANES)] * 2
    held = {"source": source, "inverse": inverse, "coupling": coupling, "base": base, "weight": weight}
    border = (f32(comps * LOW, cols), f32(comps * HIGH, cols))
    halo = f32(comps, ROWS, cols)
    for iteration in range(ITERS):
        arrived = lax.ppermute(sums, ("group", "blk"), swap)
        arrived = lax.all_to_all(arrived, "blk", split_axis=0, concat_axis=0, tiled=True)
        below = lax.ppermute(top, "blk", up)
        above = lax.ppermute(bottom, "blk", down)
        is_last = iteration == ITERS - 1
        if iteration == 0:
            cells_of = jax.ShapeDtypeStruct((blocks, slots), jnp.int32)
            (movable,) = call(
                frozen_kernel, (target,), (), (f32(rows, cols),), [vmem_like(rows, cols)]
            )
            held["low"], held["high"], low_target, high_target, below, above = call(
                partial(unpack_kernel, comps=comps, rows=rows),
                (below, above),
                (),
                (f32(fixed, ROWS, cols), f32(fixed, ROWS, cols), cells_of, cells_of, *border),
                [vmem_like((cols // LANES) * (ROWS // 2), 2 * LANES), vmem_like(1, ROWS, cols)],
            )
        names = tuple(held)
        near = tuple(pltpu.VMEM(held[name].shape, held[name].dtype) for name in names)
        state, placed_below, placed_above, *near = call(
            lambda *refs: place_kernel(len(names), refs),
            (arrived, target, state, movable, low_target, high_target),
            tuple(held[name] for name in names),
            (cells, halo, halo, *near),
            placing + [pltpu.SemaphoreType.DMA((len(names),))],
        )
        results = call(
            lambda *refs: step_kernel(names, is_last, refs),
            (state, below, above, placed_below, placed_above, movable, *near),
            (),
            (cells,) if is_last else (cells, sums_shape, *border),
            working,
        )
        state = results[0]
        if not is_last:
            sums, top, bottom = results[1:]
    return state[None, None]


def solution(mesh):
    in_specs = (
        P("group", "blk", None, None, None),
        P("group", "blk", None, None, None),
        P("group", "blk", None, None, None, None),
        P("group", "blk", None, None, None),
        P("group", "blk", None, None),
        P("group", "blk", None, None, None),
        P("group", "blk", None, None),
    )
    out_specs = P("group", "blk", None, None, None)
    return jax.shard_map(
        on_device, mesh=mesh, in_specs=in_specs, out_specs=out_specs, check_vma=False
    )
```
